32 devices in a mesh: tm: 4 (over y, x), tile: 8 (over z, core).
Axes of the slice: x: 2, y: 2, z: 4, core: 2. Of those that a mesh axis runs over, the one named last changes fastest.
Arguments:
- frames: bfloat16 [16, 32, 128, 256], P('tm', 'tile'), may hold values from -20 to 20
- first_gain: float32 [256], replicated, may hold values from 0.1 to 1.9
- first_bias: float32 [256], replicated, may hold values from -3 to 3
- first_weight: bfloat16 [3, 3, 3, 256, 256], replicated, may hold values from -0.078125 to 0.078125
- second_gain: float32 [256], replicated, may hold values from 0.1 to 1.9
- second_bias: float32 [256], replicated, may hold values from -3 to 3
- second_weight: bfloat16 [3, 3, 3, 256, 256], replicated, may hold values from -0.1875 to 0.1875
- latent_weight: bfloat16 [256, 16], replicated, may hold values from -0.375 to 0.375
Outputs:
- features: bfloat16 [16, 32, 128, 256], P('tm', 'tile')
- tokens: bfloat16 [16, 16, 4096], P('tm', None, 'tile')
The draws below stay inside these ranges and needn't reach their ends.
All inputs are finite; a program needn't handle non-finite values.
Results may differ from the reference program's by a relative error of at most 0.012.
Values may be sent and summed in bfloat16 or wider, within the bound.
No kernel may reach another device: no remote copies, remote signals or barrier semaphores. Data moves between devices by JAX's collectives and lax.ppermute only.
A program may use at most 128 MiB of HBM per device.

```python
import jax
import jax.numpy as jnp
from jax import lax

C = 256
GROUPS = 32
LAT = 16
W = 128
NT = 16
NH = 32


def draw_frames(key, part):
    time_ramp = jnp.arange(NT, dtype=jnp.float32) / max(NT - 1, 1)
    row_ramp = jnp.arange(NH, dtype=jnp.float32) / max(NH - 1, 1)
    growth = jnp.exp(0.5 * jnp.log(3.0) * (time_ramp[:, None] + row_ramp[None, :]))[:, :, None, None]
    extent = (NT, NH, W, C)
    drawn = jax.random.truncated_normal(jax.random.fold_in(key, 13), -4.0, 4.0, extent, jnp.float32) * growth
    return drawn.astype(jnp.bfloat16)


def noise(stream_key, shape, width, reach, kind=jnp.bfloat16):
    result = width * jax.random.normal(stream_key, shape, jnp.float32)
    return jnp.clip(result, min=-reach, max=reach).astype(kind)


def setup_inputs(seed: int = 0) -> dict:
    splits = jax.random.split(jax.random.key(seed), 9)
    frames = draw_frames(jax.random.fold_in(splits[8], 71), 0)
    first_gain = jnp.clip(1.0 + 0.18 * jax.random.normal(splits[1], (C,), jnp.float32), 0.1, 1.9)
    first_bias = noise(splits[2], (C,), 0.5, 3.0, jnp.float32)
    first_weight = noise(splits[3], (3, 3, 3, C, C), (27 * C) ** -0.5, 0.078125)
    second_gain = jnp.clip(1.0 + 0.18 * jax.random.normal(splits[4], (C,), jnp.float32), 0.1, 1.9)
    second_bias = noise(splits[5], (C,), 0.5, 3.0, jnp.float32)
    second_weight = noise(splits[6], (3, 3, 3, C, C), (2.5 * (27 * C) ** -0.5), 0.1875)
    latent_weight = noise(splits[7], (C, LAT), C ** -0.5, 0.375)
    return {"frames": frames, "first_gain": first_gain, "first_bias": first_bias, "first_weight": first_weight, "second_gain": second_gain, "second_bias": second_bias, "second_weight": second_weight, "latent_weight": latent_weight}


def normalize(values, members, gain, bias):
    sums = lax.optimization_barrier(jnp.sum(values, axis=(0, 1, 2))).reshape(GROUPS, -1).sum(axis=1)
    squares = lax.optimization_barrier(jnp.sum(values * values, axis=(0, 1, 2))).reshape(GROUPS, -1).sum(axis=1)
    average = sums / members
    spread = squares / members - average * average
    inverse = lax.rsqrt(spread + 1e-06)
    factor = jnp.repeat(inverse, C // GROUPS) * gain
    offset = bias - jnp.repeat(average, C // GROUPS) * factor
    return jax.nn.silu(values * factor + offset).astype(jnp.bfloat16)

def causal_conv(active, kernel):
    convolved = lax.conv_general_dilated(active[None], kernel, (1, 1, 1), [(2, 0), (1, 1), (1, 1)], dimension_numbers=('NDHWC', 'DHWIO', 'NDHWC'), preferred_element_type=jnp.float32)
    return convolved[0]

def reference(frames, first_gain, first_bias, first_weight, second_gain, second_bias, second_weight, latent_weight):
    members = float(NT * NH * W * (C // GROUPS))
    inputs = frames.astype(jnp.float32)
    active = normalize(inputs, members, first_gain, first_bias)
    hidden = causal_conv(active, first_weight).astype(jnp.bfloat16)
    active = normalize(hidden.astype(jnp.float32), members, second_gain, second_bias)
    branch = causal_conv(active, second_weight)
    features = (inputs + branch).astype(jnp.bfloat16)
    latents = jnp.dot(features.reshape(-1, C), latent_weight, preferred_element_type=jnp.float32).astype(jnp.bfloat16)
    tokens = latents.reshape(NT, NH // 2, 2, W // 2, 2, LAT).transpose(0, 1, 3, 2, 4, 5).reshape(NT, NH // 2, -1)
    return (features, tokens)
```

```python
import functools

import jax
import jax.numpy as jnp
from jax import lax
from jax.experimental import pallas as pl
from jax.experimental.pallas import tpu as pltpu
from jax.sharding import PartitionSpec as P

GROUPS = 32
ALL = ("tm", "tile")
VMEM = pl.BlockSpec(memory_space=pltpu.VMEM)
LANES = 128


def params(mib):
    return pltpu.CompilerParams(vmem_limit_bytes=mib << 20)


def row_totals(value):
    folded = value.reshape(-1, 8, value.shape[-1])
    return jnp.sum(folded, axis=0)


def put_stats(out_ref, sums, squares):
    pair = jnp.concatenate(
        [jnp.sum(sums, axis=0, keepdims=True), jnp.sum(squares, axis=0, keepdims=True)], axis=0
    )
    out_ref[...] = jnp.broadcast_to(pair[None], out_ref.shape)


def stats_kernel(frames_ref, out_ref):
    depth, height, columns, channels = frames_ref.shape

    def step(t, carry):
        sums, squares = carry
        for h in range(height):
            value = frames_ref[t, h].astype(jnp.float32)
            sums = sums + row_totals(value)
            squares = squares + row_totals(value * value)
        return sums, squares

    zero = jnp.zeros((8, channels), jnp.float32)
    sums, squares = lax.fori_loop(0, depth, step, (zero, zero))
    put_stats(out_ref, sums, squares)


def group_sum(value, size):
    channels = value.shape[1]
    lane = lax.broadcasted_iota(jnp.int32, value.shape, 1)
    step = 1
    while step < size:
        ahead = pltpu.roll(value, channels - step, 1)
        behind = pltpu.roll(value, step, 1)
        value = value + jnp.where((lane // step) % 2 == 0, ahead, behind)
        step *= 2
    return value


def scale_of(stats_ref, gain_ref, bias_ref, members):
    channels = stats_ref.shape[2]
    totals = jnp.sum(stats_ref[...], axis=0)
    totals = jnp.concatenate([totals, jnp.zeros((6, channels), jnp.float32)], axis=0)
    totals = group_sum(totals, channels // GROUPS)
    average = totals[0:1] / members
    spread = totals[1:2] / members - average * average
    factor = lax.rsqrt(spread + 1e-06) * gain_ref[...]
    return factor, bias_ref[...] - average * factor


def silu(value):
    return value * (0.5 * jnp.tanh(0.5 * value) + 0.5)


def fill(active_ref, own_ref, past_ref, top_ref, bottom_ref, ctop_ref, cbottom_ref, scale):
    factor, offset = scale
    depth, height = own_ref.shape[:2]
    row = lax.axis_index("tile")
    first = (lax.axis_index("tm") > 0).astype(jnp.float32)
    above = (row > 0).astype(jnp.float32)
    below = (row < lax.axis_size("tile") - 1).astype(jnp.float32)

    def put(t, h, value, keep):
        active = silu(value.astype(jnp.float32) * factor + offset)
        if keep is not None:
            active = active * keep
        active_ref[t, h] = active.astype(jnp.bfloat16)

    def past(t, carry):
        put(t, 0, ctop_ref[t, 0], first * above)
        for h in range(height):
            put(t, h + 1, past_ref[t, h], first)
        put(t, height + 1, cbottom_ref[t, 0], first * below)
        return carry

    def own(t, carry):
        put(t + 2, 0, top_ref[t, 0], above)
        for h in range(height):
            put(t + 2, h + 1, own_ref[t, h], None)
        put(t + 2, height + 1, bottom_ref[t, 0], below)
        return carry

    lax.fori_loop(0, 2, past, 0)
    lax.fori_loop(0, depth, own, 0)


def convolve(active_ref, weight_ref, t, height):
    columns, channels = active_ref.shape[2:]
    rows = height * columns
    totals = []
    for c in range(3):
        total = None
        for a in range(3):
            for b in range(3):
                piece = active_ref[t + a, b : b + height].reshape(rows, channels)
                part = jnp.dot(piece, weight_ref[a, b, c], preferred_element_type=jnp.float32)
                total = part if total is None else total + part
        totals.append(total)
    column = lax.broadcasted_iota(jnp.int32, totals[0].shape, 0) % columns
    left = jnp.where(column == 0, 0.0, pltpu.roll(totals[0], 1, 0))
    right = jnp.where(column == columns - 1, 0.0, pltpu.roll(totals[2], rows - 1, 0))
    return totals[1] + left + right


def first_kernel(members, own, past, top, bottom, ctop, cbottom, stats, gain, bias, weight,
                 hidden_ref, out_stats_ref, active_ref):
    depth, height, columns, channels = own.shape
    fill(active_ref, own, past, top, bottom, ctop, cbottom, scale_of(stats, gain, bias, members))

    def step(t, carry):
        sums, squares = carry
        hidden = convolve(active_ref, weight, t, height).astype(jnp.bfloat16)
        hidden_ref[t] = hidden.reshape(height, columns, channels)
        wide = hidden.astype(jnp.float32)
        return sums + row_totals(wide), squares + row_totals(wide * wide)

    zero = jnp.zeros((8, channels), jnp.float32)
    sums, squares = lax.fori_loop(0, depth, step, (zero, zero))
    put_stats(out_stats_ref, sums, squares)


def second_kernel(members, own, past, top, bottom, ctop, cbottom, stats, gain, bias, weight,
                  frames, latent, features_ref, patches_ref, active_ref, latents_ref, packed_ref):
    depth, height, columns, channels = own.shape
    width = LANES // 8
    fill(active_ref, own, past, top, bottom, ctop, cbottom, scale_of(stats, gain, bias, members))
    parts, rows = packed_ref.shape[:2]
    pairs = height // 2
    blocks = rows // (depth * pairs)
    lane = lax.broadcasted_iota(jnp.int32, (columns // 4, LANES), 1) // width

    def step(t, carry):
        branch = convolve(active_ref, weight, t, height)
        residual = frames[t].reshape(height * columns, channels).astype(jnp.float32)
        features = (residual + branch).astype(jnp.bfloat16)
        features_ref[t] = features.reshape(height, columns, channels)
        latents_ref[...] = (
            jnp.dot(features, latent[...], preferred_element_type=jnp.float32)
            .astype(jnp.bfloat16)
            .astype(jnp.float32)
        )
        for i in range(pairs):
            mixed = None
            for cell in range(8):
                j, p, q = cell // 4, cell // 2 % 2, cell % 2
                start = (2 * i + p) * columns + 2 * j + q
                value = latents_ref[pl.ds(start, columns // 4, stride=4), :]
                mixed = value if mixed is None else jnp.where(lane == cell, value, mixed)
            for d in range(parts):
                packed_ref[d, pl.ds(t * blocks * pairs + i, blocks, stride=pairs), :] = mixed[
                    d * blocks : (d + 1) * blocks
                ]
        return carry

    lax.fori_loop(0, depth, step, 0)
    patches_ref[...] = packed_ref[...].astype(jnp.bfloat16)


def unpack_kernel(blocks, pairs, received, tokens_ref, flat_ref, mixed_ref):
    parts, rows, lanes = received.shape
    flat_ref[...] = received[...].astype(jnp.float32).reshape(parts * rows, lanes)
    depth = rows // (blocks * pairs)
    for t in range(depth):
        for block in range(blocks):
            for i in range(pairs):
                start = (t * blocks + block) * pairs + i
                mixed_ref[t * blocks + block, pl.ds(i, parts, stride=pairs), :] = flat_ref[
                    pl.ds(start, parts, stride=rows), :
                ]
            tokens_ref[t, :, block * lanes : (block + 1) * lanes] = mixed_ref[
                t * blocks + block
            ].astype(jnp.bfloat16)


def surround(cells):
    depth, height = cells.shape[:2]
    frames, rows = lax.axis_size("tm"), lax.axis_size("tile")

    def moved(value, down, right):
        pairs = []
        for i in range(frames):
            for j in range(rows):
                if 0 <= i + down < frames and 0 <= j + right < rows:
                    pairs.append((i * rows + j, (i + down) * rows + j + right))
        return lax.ppermute(value, ALL, pairs)

    first, last = cells[:, :1], cells[:, height - 1 :]
    past = moved(cells[depth - 2 :], 1, 0)
    top = moved(last, 0, 1)
    bottom = moved(first, 0, -1)
    ctop = moved(last[depth - 2 :], 1, 1)
    cbottom = moved(first[depth - 2 :], 1, -1)
    return past, top, bottom, ctop, cbottom


def exchange(stats):
    return lax.all_to_all(stats, ALL, split_axis=0, concat_axis=0, tiled=True)


def body(frames, first_gain, first_bias, first_weight, second_gain, second_bias, second_weight,
         latent_weight):
    depth, height, columns, channels = frames.shape
    parts = lax.axis_size("tile")
    devices = lax.axis_size("tm") * parts
    members = float(devices * depth * height * columns * (channels // GROUPS))
    latent_width = latent_weight.shape[1]
    pairs = height // 2
    blocks = columns // 2 * 4 * latent_width // parts // LANES
    rows = depth * blocks * pairs
    stats_shape = jax.ShapeDtypeStruct((devices, 2, channels), jnp.float32)
    cells_shape = jax.ShapeDtypeStruct(frames.shape, jnp.bfloat16)
    active = pltpu.VMEM((depth + 2, height + 2, columns, channels), jnp.bfloat16)
    flops = 2 * 27 * depth * height * columns * channels * channels
    cost = pl.CostEstimate(flops=flops, bytes_accessed=8 << 20, transcendentals=0)

    stats = pl.pallas_call(
        stats_kernel, out_shape=stats_shape, in_specs=[VMEM], out_specs=VMEM,
        compiler_params=params(16), name="stats",
    )(frames)
    around = surround(frames)
    stats = exchange(stats)
    hidden, stats = pl.pallas_call(
        functools.partial(first_kernel, members), out_shape=(cells_shape, stats_shape),
        in_specs=[VMEM] * 10, out_specs=(VMEM, VMEM), scratch_shapes=[active],
        compiler_params=params(40), cost_estimate=cost, name="first",
    )(frames, *around, stats, first_gain[None], first_bias[None], first_weight)
    around = surround(hidden)
    stats = exchange(stats)
    wide_latent = jnp.tile(latent_weight, (1, LANES // latent_width))
    features, patches = pl.pallas_call(
        functools.partial(second_kernel, members),
        out_shape=(cells_shape, jax.ShapeDtypeStruct((parts, rows, LANES), jnp.bfloat16)),
        in_specs=[VMEM] * 12, out_specs=(VMEM, VMEM),
        scratch_shapes=[active, pltpu.VMEM((height * columns, LANES), jnp.float32),
                        pltpu.VMEM((parts, rows, LANES), jnp.float32)],
        compiler_params=params(40), cost_estimate=cost, name="second",
    )(hidden, *around, stats, second_gain[None], second_bias[None], second_weight, frames,
      wide_latent)
    received = lax.all_to_all(patches, "tile", split_axis=0, concat_axis=0, tiled=True)
    tokens = pl.pallas_call(
        functools.partial(unpack_kernel, blocks, pairs),
        out_shape=jax.ShapeDtypeStruct((depth, parts * pairs, blocks * LANES), jnp.bfloat16),
        in_specs=[VMEM], out_specs=VMEM,
        scratch_shapes=[pltpu.VMEM((parts * rows, LANES), jnp.float32),
                        pltpu.VMEM((depth * blocks, parts * pairs, LANES), jnp.float32)],
        compiler_params=params(16), name="unpack",
    )(received)
    return features, tokens


def solution(mesh):
    in_specs = (P("tm", "tile", None, None), P(), P(), P(), P(), P(), P(), P())
    out_specs = (P("tm", "tile", None, None), P("tm", None, "tile"))
    return jax.shard_map(body, mesh=mesh, in_specs=in_specs, out_specs=out_specs, check_vma=False)
```

```python
import functools

import jax
import jax.numpy as jnp
from jax import lax
from jax.experimental import pallas as pl
from jax.experimental.pallas import tpu as pltpu
from jax.sharding import PartitionSpec as P


GROUPS = 32
ALL = ("tm", "tile")
VMEM = pl.BlockSpec(memory_space=pltpu.VMEM)
HBM = pl.BlockSpec(memory_space=pltpu.HBM)
LANES = 128


def params(mib):
    return pltpu.CompilerParams(vmem_limit_bytes=mib << 20)


def row_totals(value):
    folded = value.reshape(-1, 8, value.shape[-1])
    return jnp.sum(folded, axis=0)


def put_stats(out_ref, sums, squares):
    pair = jnp.concatenate(
        [jnp.sum(sums, axis=0, keepdims=True), jnp.sum(squares, axis=0, keepdims=True)], axis=0
    )
    out_ref[...] = jnp.broadcast_to(pair[None], out_ref.shape)


def stats_kernel(frames_ref, out_ref, head_ref, last_ref):
    depth, height, _, channels = frames_ref.shape

    def step(t, carry):
        sums, squares = carry
        for h in range(height):
            value = frames_ref[t, h].astype(jnp.float32)
            sums = sums + row_totals(value)
            squares = squares + row_totals(value * value)
        return sums, squares

    zero = jnp.zeros((8, channels), jnp.float32)
    sums, squares = lax.fori_loop(0, depth, step, (zero, zero))
    put_stats(out_ref, sums, squares)
    head_ref[...] = frames_ref[: depth - 2]
    last_ref[...] = frames_ref[depth - 2 :]


def pick_kernel(past_ref, *refs):
    *own_refs, near_ref, far_ref = refs
    height = past_ref.shape[1]
    even = lax.axis_index("tile") % 2 == 0
    near = jnp.where(even, height - 1, 0)
    far = jnp.where(even, 0, height - 1)
    t = 0
    for ref in (past_ref, *own_refs):
        for frame in range(ref.shape[0]):
            near_ref[t] = ref[frame, near]
            far_ref[t] = ref[frame, far]
            t += 1


def group_sum(value, size):
    channels = value.shape[1]
    lane = lax.broadcasted_iota(jnp.int32, value.shape, 1)
    step = 1
    while step < size:
        ahead = pltpu.roll(value, channels - step, 1)
        behind = pltpu.roll(value, step, 1)
        value = value + jnp.where((lane // step) % 2 == 0, ahead, behind)
        step *= 2
    return value


def scale_of(stats_ref, gain_ref, bias_ref, members):
    channels = stats_ref.shape[2]
    totals = jnp.sum(stats_ref[...], axis=0)
    totals = jnp.concatenate([totals, jnp.zeros((6, channels), jnp.float32)], axis=0)
    totals = group_sum(totals, channels // GROUPS)
    average = totals[0:1] / members
    spread = totals[1:2] / members - average * average
    factor = lax.rsqrt(spread + 1e-06) * gain_ref[...]
    return factor, bias_ref[...] - average * factor


def silu(value):
    return value * (0.5 * jnp.tanh(0.5 * value) + 0.5)


def fill(active_ref, begin, past_ref, own_refs, near_ref, far_ref, scale):
    factor, offset = scale
    height = past_ref.shape[1]
    index, count = lax.axis_index("tile"), lax.axis_size("tile")
    even = index % 2 == 0
    first = (lax.axis_index("tm") > 0).astype(jnp.float32)
    near_row, far_row = jnp.where(even, height + 1, 0), jnp.where(even, 0, height + 1)
    above, below = index > 0, index < count - 1
    near_keep = jnp.where(even, below, above).astype(jnp.float32)
    far_keep = jnp.where(even, above, below).astype(jnp.float32)

    def put(t, h, value, keep):
        active = silu(value.astype(jnp.float32) * factor + offset)
        if keep is not None:
            active = active * keep
        active_ref[t, h] = active.astype(jnp.bfloat16)

    frame = 0
    for ref in (past_ref, *own_refs):
        skip = max(0, begin - frame)

        def one(t, carry, ref=ref, frame=frame):
            keep = first if ref is past_ref else None
            place = frame + t - begin
            for h in range(height):
                put(place, h + 1, ref[t, h], keep)
            put(place, near_row, near_ref[frame + t], near_keep if keep is None else near_keep * keep)
            put(place, far_row, far_ref[frame + t], far_keep if keep is None else far_keep * keep)
            return carry

        stop = min(ref.shape[0], active_ref.shape[0] + begin - frame)
        if stop > skip:
            lax.fori_loop(skip, stop, one, 0)
        frame += ref.shape[0]


def weight_copies(weight_hbm, weight_ref, sem):
    return [
        pltpu.make_async_copy(weight_hbm.at[:, :, c], weight_ref.at[c], sem.at[c]) for c in range(3)
    ]


def convolve(active_ref, weight_ref, t, height, copies):
    columns, channels = active_ref.shape[2:]
    rows = height * columns
    totals = []
    for c in range(3):
        pl.when(t == 0)(copies[c].wait)
        total = None
        for a in range(3):
            for b in range(3):
                piece = active_ref[t + a, b : b + height].reshape(rows, channels)
                part = jnp.dot(piece, weight_ref[c, a, b], preferred_element_type=jnp.float32)
                total = part if total is None else total + part
        totals.append(total)
    column = lax.broadcasted_iota(jnp.int32, totals[0].shape, 0) % columns
    left = jnp.where(column == 0, 0.0, pltpu.roll(totals[0], 1, 0))
    right = jnp.where(column == columns - 1, 0.0, pltpu.roll(totals[2], rows - 1, 0))
    return totals[1] + left + right


def first_kernel(members, begin, owns, more, past, *refs):
    own, refs = refs[:owns], refs[owns:]
    near, far, stats, gain, bias, weight = refs[:6]
    hidden_ref, totals_ref, active_ref, weight_ref, sem = refs[-5:]
    depth, height, columns, channels = hidden_ref.shape
    copies = weight_copies(weight, weight_ref, sem)
    for copy in copies:
        copy.start()
    fill(active_ref, begin, past, own, near, far, scale_of(stats, gain, bias, members))

    def step(t, carry):
        sums, squares = carry
        hidden = convolve(active_ref, weight_ref, t, height, copies).astype(jnp.bfloat16)
        hidden_ref[t] = hidden.reshape(height, columns, channels)
        wide = hidden.astype(jnp.float32)
        return sums + row_totals(wide), squares + row_totals(wide * wide)

    zero = jnp.zeros((8, channels), jnp.float32)
    start = (refs[6][0], refs[6][1]) if more else (zero, zero)
    sums, squares = lax.fori_loop(0, depth, step, start)
    if more:
        put_stats(totals_ref, sums, squares)
    else:
        totals_ref[0] = sums
        totals_ref[1] = squares


def second_kernel(members, owns, past, *refs):
    own, refs = refs[:owns], refs[owns:]
    near, far, stats, gain, bias, weight, frames, latent = refs[:8]
    features_hbm, patches_ref, active_ref, latents_ref, packed_ref = refs[8:13]
    weight_ref, cells_ref, sem, in_sem, out_sem = refs[13:]
    depth, height, columns, channels = frames.shape
    copies = weight_copies(weight, weight_ref, sem)
    for copy in copies:
        copy.start()
    loads = pltpu.make_async_copy(frames, cells_ref, in_sem)
    loads.start()
    width = LANES // 8
    fill(active_ref, 0, past, own, near, far, scale_of(stats, gain, bias, members))
    parts, rows = packed_ref.shape[:2]
    pairs = height // 2
    blocks = rows // (depth * pairs)
    lane = lax.broadcasted_iota(jnp.int32, (columns // 4, LANES), 1) // width
    spread = lax.broadcasted_iota(jnp.int32, (width, LANES), 0) == (
        lax.broadcasted_iota(jnp.int32, (width, LANES), 1) % width
    )
    wide_latent = lax.dot_general(
        latent[...], spread.astype(jnp.bfloat16), (((0,), (0,)), ((), ())),
        preferred_element_type=jnp.float32,
    ).astype(jnp.bfloat16)

    def step(t, carry):
        branch = convolve(active_ref, weight_ref, t, height, copies)
        pl.when(t == 0)(loads.wait)
        residual = cells_ref[t].reshape(height * columns, channels).astype(jnp.float32)
        features = (residual + branch).astype(jnp.bfloat16)
        cells_ref[t] = features.reshape(height, columns, channels)
        pltpu.make_async_copy(cells_ref.at[t], features_hbm.at[t], out_sem.at[t]).start()
        latents_ref[...] = (
            jnp.dot(features, wide_latent, preferred_element_type=jnp.float32)
            .astype(jnp.bfloat16)
            .astype(jnp.float32)
        )
        for i in range(pairs):
            mixed = None
            for cell in range(8):
                j, p, q = cell // 4, cell // 2 % 2, cell % 2
                start = (2 * i + p) * columns + 2 * j + q
                value = latents_ref[pl.ds(start, columns // 4, stride=4), :]
                mixed = value if mixed is None else jnp.where(lane == cell, value, mixed)
            for d in range(parts):
                packed_ref[d, pl.ds(t * blocks * pairs + i, blocks, stride=pairs), :] = mixed[
                    d * blocks : (d + 1) * blocks
                ]
        return carry

    lax.fori_loop(0, depth, step, 0)
    patches_ref[...] = packed_ref[...].astype(jnp.bfloat16)
    for t in range(depth):
        pltpu.make_async_copy(cells_ref.at[t], features_hbm.at[t], out_sem.at[t]).wait()


def unpack_kernel(blocks, pairs, received, tokens_ref, flat_ref, mixed_ref):
    parts, rows, lanes = received.shape
    flat_ref[...] = received[...].astype(jnp.float32).reshape(parts * rows, lanes)
    depth = rows // (blocks * pairs)
    for t in range(depth):
        for block in range(blocks):
            for i in range(pairs):
                start = (t * blocks + block) * pairs + i
                mixed_ref[t * blocks + block, pl.ds(i, parts, stride=pairs), :] = flat_ref[
                    pl.ds(start, parts, stride=rows), :
                ]
            tokens_ref[t, :, block * lanes : (block + 1) * lanes] = mixed_ref[
                t * blocks + block
            ].astype(jnp.bfloat16)


def ahead_pairs():
    return [(i, i + 1) for i in range(lax.axis_size("tm") - 1)]


def surround(last, own):
    past = lax.ppermute(last, "tm", ahead_pairs())
    _, columns, channels = last.shape[1:]
    count = lax.axis_size("tile")
    near_pairs = [(i, i ^ 1) for i in range(count) if i ^ 1 < count]
    far_pairs = [pair for i in range(1, count - 1, 2) for pair in ((i, i + 1), (i + 1, i))]
    rows = jax.ShapeDtypeStruct(
        (2 + sum(piece.shape[0] for piece in own), columns, channels), jnp.bfloat16
    )
    near, far = pl.pallas_call(
        pick_kernel, out_shape=(rows, rows), in_specs=[VMEM] * (1 + len(own)),
        out_specs=(VMEM, VMEM), compiler_params=params(8), name="pick",
    )(past, *own)
    near = lax.ppermute(near, "tile", near_pairs)
    far = lax.ppermute(far, "tile", far_pairs)
    return past, *own, near, far


def exchange(stats):
    return lax.all_to_all(stats, ALL, split_axis=0, concat_axis=0, tiled=True)


def body(frames, first_gain, first_bias, first_weight, second_gain, second_bias, second_weight,
         latent_weight):
    depth, height, columns, channels = frames.shape
    parts = lax.axis_size("tile")
    devices = lax.axis_size("tm") * parts
    members = float(devices * depth * height * columns * (channels // GROUPS))
    latent_width = latent_weight.shape[1]
    pairs = height // 2
    blocks = columns // 2 * 4 * latent_width // parts // LANES
    rows = depth * blocks * pairs
    stats_shape = jax.ShapeDtypeStruct((devices, 2, channels), jnp.float32)
    cells_shape = jax.ShapeDtypeStruct(frames.shape, jnp.bfloat16)
    last_shape = jax.ShapeDtypeStruct((2, *frames.shape[1:]), jnp.bfloat16)
    head_shape = jax.ShapeDtypeStruct((depth - 2, *frames.shape[1:]), jnp.bfloat16)

    weights = [pltpu.VMEM((3, 3, 3, channels, channels), jnp.bfloat16), pltpu.SemaphoreType.DMA((3,))]

    def active(count):
        return [pltpu.VMEM((count + 2, height + 2, columns, channels), jnp.bfloat16), *weights]

    def cost(count):
        flops = 2 * 27 * count * height * columns * channels * channels
        return pl.CostEstimate(flops=flops, bytes_accessed=8 << 20, transcendentals=0)

    first_weight = pltpu.with_memory_space_constraint(first_weight, pltpu.HBM)
    second_weight = pltpu.with_memory_space_constraint(second_weight, pltpu.HBM)
    cells = pltpu.with_memory_space_constraint(frames, pltpu.HBM)
    stats, head, last = pl.pallas_call(
        stats_kernel, out_shape=(stats_shape, head_shape, last_shape), in_specs=[VMEM],
        out_specs=(VMEM, VMEM, VMEM), compiler_params=params(8), cost_estimate=cost(1), name="stats",
    )(frames)
    around = surround(last, (head, last))
    stats = exchange(stats)
    operands = (*around, stats, first_gain[None], first_bias[None], first_weight)
    last, totals = pl.pallas_call(
        functools.partial(first_kernel, members, depth - 2, 2, False),
        out_shape=(last_shape, jax.ShapeDtypeStruct((2, 8, channels), jnp.float32)),
        in_specs=[VMEM] * 8 + [HBM], out_specs=(VMEM, VMEM), scratch_shapes=active(2),
        compiler_params=params(24), cost_estimate=cost(2), name="first_last",
    )(*operands)
    head, stats = pl.pallas_call(
        functools.partial(first_kernel, members, 0, 2, True),
        out_shape=(head_shape, stats_shape),
        in_specs=[VMEM] * 8 + [HBM, VMEM], out_specs=(VMEM, VMEM), scratch_shapes=active(depth - 2),
        compiler_params=params(24), cost_estimate=cost(depth - 2), name="first_head",
    )(*operands, totals)
    around = surround(last, (head, last))
    stats = exchange(stats)
    features, patches = pl.pallas_call(
        functools.partial(second_kernel, members, 2),
        out_shape=(cells_shape, jax.ShapeDtypeStruct((parts, rows, LANES), jnp.bfloat16)),
        in_specs=[VMEM] * 8 + [HBM, HBM, VMEM], out_specs=(HBM, VMEM),
        scratch_shapes=[active(depth)[0], pltpu.VMEM((height * columns, LANES), jnp.float32),
                        pltpu.VMEM((parts, rows, LANES), jnp.float32), weights[0],
                        pltpu.VMEM(frames.shape, jnp.bfloat16), weights[1],
                        pltpu.SemaphoreType.DMA(()), pltpu.SemaphoreType.DMA((depth,))],
        compiler_params=params(24), cost_estimate=cost(depth), name="second",
    )(*around, stats, second_gain[None], second_bias[None], second_weight, cells, latent_weight.T)
    received = lax.all_to_all(patches, "tile", split_axis=0, concat_axis=0, tiled=True)
    tokens = pl.pallas_call(
        functools.partial(unpack_kernel, blocks, pairs),
        out_shape=jax.ShapeDtypeStruct((depth, parts * pairs, blocks * LANES), jnp.bfloat16),
        in_specs=[VMEM], out_specs=VMEM,
        scratch_shapes=[pltpu.VMEM((parts * rows, LANES), jnp.float32),
                        pltpu.VMEM((depth * blocks, parts * pairs, LANES), jnp.float32)],
        compiler_params=params(16), name="unpack",
    )(received)
    return features, tokens


def solution(mesh):
    in_specs = (P("tm", "tile", None, None), P(), P(), P(), P(), P(), P(), P())
    out_specs = (P("tm", "tile", None, None), P("tm", None, "tile"))
    return jax.shard_map(body, mesh=mesh, in_specs=in_specs, out_specs=out_specs, check_vma=False)
```

```python
import functools

import jax
import jax.numpy as jnp
from jax import lax
from jax.experimental import pallas as pl
from jax.experimental.pallas import tpu as pltpu
from jax.sharding import PartitionSpec as P


GROUPS = 32
ALL = ("tm", "tile")
VMEM = pl.BlockSpec(memory_space=pltpu.VMEM)
HBM = pl.BlockSpec(memory_space=pltpu.HBM)
LANES = 128


def params(mib):
    return pltpu.CompilerParams(vmem_limit_bytes=mib << 20)


def row_totals(value):
    folded = value.reshape(-1, 8, value.shape[-1])
    return jnp.sum(folded, axis=0)


def put_stats(out_ref, sums, squares):
    pair = jnp.concatenate(
        [jnp.sum(sums, axis=0, keepdims=True), jnp.sum(squares, axis=0, keepdims=True)], axis=0
    )
    out_ref[...] = jnp.broadcast_to(pair[None], out_ref.shape)


def sides(height):
    even = lax.axis_index("tile") % 2 == 0
    return jnp.where(even, height - 1, 0), jnp.where(even, 0, height - 1)


def stats_kernel(frames_ref, out_ref, head_ref, last_ref, near_ref, far_ref):
    depth, height, _, channels = frames_ref.shape
    near, far = sides(height)

    def step(t, carry):
        sums, squares = carry
        for h in range(height):
            value = frames_ref[t, h].astype(jnp.float32)
            sums = sums + row_totals(value)
            squares = squares + row_totals(value * value)
        near_ref[t] = frames_ref[t, near]
        far_ref[t] = frames_ref[t, far]
        return sums, squares

    zero = jnp.zeros((8, channels), jnp.float32)
    sums, squares = lax.fori_loop(0, depth, step, (zero, zero))
    put_stats(out_ref, sums, squares)
    head_ref[...] = frames_ref[: depth - 2]
    last_ref[...] = frames_ref[depth - 2 :]


def pick_kernel(count, *refs):
    cell_refs, (near_ref, far_ref) = refs[:count], refs[-2:]
    near, far = sides(cell_refs[0].shape[1])
    t = 0
    for ref in cell_refs:
        for frame in range(ref.shape[0]):
            near_ref[t] = ref[frame, near]
            far_ref[t] = ref[frame, far]
            t += 1


def group_sum(value, size):
    channels = value.shape[1]
    lane = lax.broadcasted_iota(jnp.int32, value.shape, 1)
    step = 1
    while step < size:
        ahead = pltpu.roll(value, channels - step, 1)
        behind = pltpu.roll(value, step, 1)
        value = value + jnp.where((lane // step) % 2 == 0, ahead, behind)
        step *= 2
    return value


def scale_of(stats_ref, gain_ref, bias_ref, members):
    channels = stats_ref.shape[2]
    totals = jnp.sum(stats_ref[...], axis=0)
    totals = jnp.concatenate([totals, jnp.zeros((6, channels), jnp.float32)], axis=0)
    totals = group_sum(totals, channels // GROUPS)
    average = totals[0:1] / members
    spread = totals[1:2] / members - average * average
    factor = lax.rsqrt(spread + 1e-06) * gain_ref[...]
    return factor, bias_ref[...] - average * factor


def silu(value):
    return value * (0.5 * jnp.tanh(0.5 * value) + 0.5)


def fill(active_ref, begin, pieces, scale):
    factor, offset = scale
    height = active_ref.shape[1] - 2
    index, count = lax.axis_index("tile"), lax.axis_size("tile")
    even = index % 2 == 0
    first = (lax.axis_index("tm") > 0).astype(jnp.float32)
    near_row, far_row = jnp.where(even, height + 1, 0), jnp.where(even, 0, height + 1)
    above, below = index > 0, index < count - 1
    near_keep = jnp.where(even, below, above).astype(jnp.float32)
    far_keep = jnp.where(even, above, below).astype(jnp.float32)

    def put(t, h, value, keep):
        active = silu(value.astype(jnp.float32) * factor + offset)
        if keep is not None:
            active = active * keep
        active_ref[t, h] = active.astype(jnp.bfloat16)

    for frame, ref, near_ref, far_ref, shift, is_past in pieces:
        skip = max(0, begin - frame)
        stop = min(ref.shape[0], active_ref.shape[0] + begin - frame)

        def one(t, carry):
            place = frame + t - begin
            for h in range(height):
                put(place, h + 1, ref[t, h], first if is_past else None)
            put(place, near_row, near_ref[shift + t], near_keep * first if is_past else near_keep)
            put(place, far_row, far_ref[shift + t], far_keep * first if is_past else far_keep)
            return carry

        if stop > skip:
            lax.fori_loop(skip, stop, one, 0)


def convolve(active_ref, weight_ref, t, height):
    columns, channels = active_ref.shape[2:]
    rows = height * columns
    totals = []
    for c in range(3):
        total = None
        for a in range(3):
            for b in range(3):
                piece = active_ref[t + a, b : b + height].reshape(rows, channels)
                part = jnp.dot(piece, weight_ref[a, b, c], preferred_element_type=jnp.float32)
                total = part if total is None else total + part
        totals.append(total)
    column = lax.broadcasted_iota(jnp.int32, totals[0].shape, 0) % columns
    left = jnp.where(column == 0, 0.0, pltpu.roll(totals[0], 1, 0))
    right = jnp.where(column == columns - 1, 0.0, pltpu.roll(totals[2], rows - 1, 0))
    return totals[1] + left + right


def first_kernel(members, begin, with_past, with_totals, *refs):
    refs = list(refs)
    pieces = []
    if with_past:
        past, near, far = refs[:3]
        pieces.append((0, past, near, far, 0, True))
        del refs[:3]
    head, last, near, far, stats, gain, bias, weight = refs[:8]
    before = head.shape[0]
    pieces.append((2, head, near, far, 0, False))
    pieces.append((2 + before, last, near, far, before, False))
    hidden_ref, totals_ref, active_ref = refs[-3:]
    depth, height, columns, channels = hidden_ref.shape
    fill(active_ref, begin, pieces, scale_of(stats, gain, bias, members))

    def step(t, carry):
        sums, squares = carry
        hidden = convolve(active_ref, weight, t, height).astype(jnp.bfloat16)
        hidden_ref[t] = hidden.reshape(height, columns, channels)
        wide = hidden.astype(jnp.float32)
        return sums + row_totals(wide), squares + row_totals(wide * wide)

    zero = jnp.zeros((8, channels), jnp.float32)
    start = (refs[8][0], refs[8][1]) if with_totals else (zero, zero)
    sums, squares = lax.fori_loop(0, depth, step, start)
    if with_totals:
        put_stats(totals_ref, sums, squares)
    else:
        totals_ref[0] = sums
        totals_ref[1] = squares


def second_kernel(members, past, head, last, near, far, stats, gain, bias, weight, frames, latent,
                  features_hbm, patches_ref, active_ref, latents_ref, packed_ref, cells_ref,
                  in_sem, out_sem):
    depth, height, columns, channels = frames.shape
    before = head.shape[0]
    loads = pltpu.make_async_copy(frames, cells_ref, in_sem)
    loads.start()
    width = LANES // 8
    pieces = [
        (0, past, near, far, 0, True),
        (2, head, near, far, 2, False),
        (2 + before, last, near, far, 2 + before, False),
    ]
    fill(active_ref, 0, pieces, scale_of(stats, gain, bias, members))
    loads.wait()
    parts, rows = packed_ref.shape[:2]
    pairs = height // 2
    blocks = rows // (depth * pairs)
    lane = lax.broadcasted_iota(jnp.int32, (columns // 4, LANES), 1) // width
    spread = lax.broadcasted_iota(jnp.int32, (width, LANES), 0) == (
        lax.broadcasted_iota(jnp.int32, (width, LANES), 1) % width
    )
    wide_latent = lax.dot_general(
        latent[...], spread.astype(jnp.bfloat16), (((0,), (0,)), ((), ())),
        preferred_element_type=jnp.float32,
    ).astype(jnp.bfloat16)

    def step(t, carry):
        branch = convolve(active_ref, weight, t, height)
        residual = cells_ref[t].reshape(height * columns, channels).astype(jnp.float32)
        features = (residual + branch).astype(jnp.bfloat16)
        cells_ref[t] = features.reshape(height, columns, channels)
        pltpu.make_async_copy(cells_ref.at[t], features_hbm.at[t], out_sem.at[t]).start()
        latents_ref[...] = (
            jnp.dot(features, wide_latent, preferred_element_type=jnp.float32)
            .astype(jnp.bfloat16)
            .astype(jnp.float32)
        )
        for i in range(pairs):
            mixed = None
            for cell in range(8):
                j, p, q = cell // 4, cell // 2 % 2, cell % 2
                start = (2 * i + p) * columns + 2 * j + q
                value = latents_ref[pl.ds(start, columns // 4, stride=4), :]
                mixed = value if mixed is None else jnp.where(lane == cell, value, mixed)
            for d in range(parts):
                packed_ref[d, pl.ds(t * blocks * pairs + i, blocks, stride=pairs), :] = mixed[
                    d * blocks : (d + 1) * blocks
                ]
        return carry

    lax.fori_loop(0, depth, step, 0)
    patches_ref[...] = packed_ref[...].astype(jnp.bfloat16)
    for t in range(depth):
        pltpu.make_async_copy(cells_ref.at[t], features_hbm.at[t], out_sem.at[t]).wait()


def unpack_kernel(blocks, pairs, received, tokens_ref, flat_ref, mixed_ref):
    parts, rows, lanes = received.shape
    flat_ref[...] = received[...].astype(jnp.float32).reshape(parts * rows, lanes)
    depth = rows // (blocks * pairs)
    for t in range(depth):
        for block in range(blocks):
            for i in range(pairs):
                start = (t * blocks + block) * pairs + i
                mixed_ref[t * blocks + block, pl.ds(i, parts, stride=pairs), :] = flat_ref[
                    pl.ds(start, parts, stride=rows), :
                ]
            tokens_ref[t, :, block * lanes : (block + 1) * lanes] = mixed_ref[
                t * blocks + block
            ].astype(jnp.bfloat16)


def sent_ahead(last):
    pairs = [(i, i + 1) for i in range(lax.axis_size("tm") - 1)]
    return lax.ppermute(last, "tm", pairs)


def sent_sideways(near, far):
    count = lax.axis_size("tile")
    near_pairs = [(i, i ^ 1) for i in range(count) if i ^ 1 < count]
    far_pairs = [pair for i in range(1, count - 1, 2) for pair in ((i, i + 1), (i + 1, i))]
    near = lax.ppermute(near, "tile", near_pairs)
    far = lax.ppermute(far, "tile", far_pairs)
    return near, far


def pick(cells, *after):
    rows = sum(piece.shape[0] for piece in cells)
    rows = jax.ShapeDtypeStruct((rows, *cells[0].shape[2:]), jnp.bfloat16)
    return pl.pallas_call(
        functools.partial(pick_kernel, len(cells)), out_shape=(rows, rows),
        in_specs=[VMEM] * len(cells) + [pl.BlockSpec(memory_space=pl.ANY)] * len(after),
        out_specs=(VMEM, VMEM), compiler_params=params(8), name="pick",
    )(*cells, *after)


def exchange(stats):
    return lax.all_to_all(stats, ALL, split_axis=0, concat_axis=0, tiled=True)


def body(frames, first_gain, first_bias, first_weight, second_gain, second_bias, second_weight,
         latent_weight):
    depth, height, columns, channels = frames.shape
    parts = lax.axis_size("tile")
    devices = lax.axis_size("tm") * parts
    members = float(devices * depth * height * columns * (channels // GROUPS))
    latent_width = latent_weight.shape[1]
    pairs = height // 2
    blocks = columns // 2 * 4 * latent_width // parts // LANES
    rows = depth * blocks * pairs
    stats_shape = jax.ShapeDtypeStruct((devices, 2, channels), jnp.float32)
    cells_shape = jax.ShapeDtypeStruct(frames.shape, jnp.bfloat16)
    last_shape = jax.ShapeDtypeStruct((2, *frames.shape[1:]), jnp.bfloat16)
    head_shape = jax.ShapeDtypeStruct((depth - 2, *frames.shape[1:]), jnp.bfloat16)

    row_shape = jax.ShapeDtypeStruct((depth, columns, channels), jnp.bfloat16)

    def active(count):
        return pltpu.VMEM((count + 2, height + 2, columns, channels), jnp.bfloat16)

    def cost(count):
        flops = 2 * 27 * count * height * columns * channels * channels
        return pl.CostEstimate(flops=flops, bytes_accessed=8 << 20, transcendentals=0)

    cells = pltpu.with_memory_space_constraint(frames, pltpu.HBM)
    stats, head, last, near, far = pl.pallas_call(
        stats_kernel, out_shape=(stats_shape, head_shape, last_shape, row_shape, row_shape),
        in_specs=[VMEM], out_specs=(VMEM,) * 5, compiler_params=params(8), cost_estimate=cost(1),
        name="stats",
    )(frames)
    near, far = sent_sideways(near, far)
    past = sent_ahead(last)
    stats = exchange(stats)
    corner = sent_sideways(*pick((past,), stats))
    own = (head, last, near, far, stats, first_gain[None], first_bias[None], first_weight)
    around = (past, *corner)
    alone = depth >= 4
    ahead = (() if alone else around) + own
    last, totals = pl.pallas_call(
        functools.partial(first_kernel, members, depth - 2, not alone, False),
        out_shape=(last_shape, jax.ShapeDtypeStruct((2, 8, channels), jnp.float32)),
        in_specs=[VMEM] * len(ahead), out_specs=(VMEM, VMEM), scratch_shapes=[active(2)],
        compiler_params=params(24), cost_estimate=cost(2), name="first_last",
    )(*ahead)
    head, stats = pl.pallas_call(
        functools.partial(first_kernel, members, 0, True, True),
        out_shape=(head_shape, stats_shape),
        in_specs=[VMEM] * 12, out_specs=(VMEM, VMEM), scratch_shapes=[active(depth - 2)],
        compiler_params=params(24), cost_estimate=cost(depth - 2), name="first_head",
    )(*around, *own, totals)
    past = sent_ahead(last)
    near, far = sent_sideways(*pick((past, head, last)))
    stats = exchange(stats)
    features, patches = pl.pallas_call(
        functools.partial(second_kernel, members),
        out_shape=(cells_shape, jax.ShapeDtypeStruct((parts, rows, LANES), jnp.bfloat16)),
        in_specs=[VMEM] * 9 + [HBM, VMEM], out_specs=(HBM, VMEM),
        scratch_shapes=[active(depth), pltpu.VMEM((height * columns, LANES), jnp.float32),
                        pltpu.VMEM((parts, rows, LANES), jnp.float32),
                        pltpu.VMEM(frames.shape, jnp.bfloat16),
                        pltpu.SemaphoreType.DMA(()), pltpu.SemaphoreType.DMA((depth,))],
        compiler_params=params(24), cost_estimate=cost(depth), name="second",
    )(past, head, last, near, far, stats, second_gain[None], second_bias[None], second_weight,
      cells, latent_weight.T)
    received = lax.all_to_all(patches, "tile", split_axis=0, concat_axis=0, tiled=True)
    tokens = pl.pallas_call(
        functools.partial(unpack_kernel, blocks, pairs),
        out_shape=jax.ShapeDtypeStruct((depth, parts * pairs, blocks * LANES), jnp.bfloat16),
        in_specs=[VMEM], out_specs=VMEM,
        scratch_shapes=[pltpu.VMEM((parts * rows, LANES), jnp.float32),
                        pltpu.VMEM((depth * blocks, parts * pairs, LANES), jnp.float32)],
        compiler_params=params(16), name="unpack",
    )(received)
    return features, tokens


def solution(mesh):
    in_specs = (P("tm", "tile", None, None), P(), P(), P(), P(), P(), P(), P())
    out_specs = (P("tm", "tile", None, None), P("tm", None, "tile"))
    return jax.shard_map(body, mesh=mesh, in_specs=in_specs, out_specs=out_specs, check_vma=False)
```

```python
import functools

import jax
import jax.numpy as jnp
from jax import lax
from jax.experimental import pallas as pl
from jax.experimental.pallas import tpu as pltpu
from jax.sharding import PartitionSpec as P


GROUPS = 32
ALL = ("tm", "tile")
VMEM = pl.BlockSpec(memory_space=pltpu.VMEM)
HBM = pl.BlockSpec(memory_space=pltpu.HBM)
LANES = 128


def params(mib):
    return pltpu.CompilerParams(vmem_limit_bytes=mib << 20)


def row_totals(value):
    folded = value.reshape(-1, 8, value.shape[-1])
    return jnp.sum(folded, axis=0)


def put_stats(out_ref, sums, squares):
    pair = jnp.concatenate(
        [jnp.sum(sums, axis=0, keepdims=True), jnp.sum(squares, axis=0, keepdims=True)], axis=0
    )
    out_ref[...] = jnp.broadcast_to(pair[None], out_ref.shape)


def sides(height):
    even = lax.axis_index("tile") % 2 == 0
    return jnp.where(even, height - 1, 0), jnp.where(even, 0, height - 1)


def stats_kernel(frames_ref, out_ref, head_ref, last_ref, near_ref, far_ref):
    depth, height, _, channels = frames_ref.shape
    near, far = sides(height)

    def step(t, carry):
        sums, squares = carry
        for h in range(height):
            value = frames_ref[t, h].astype(jnp.float32)
            sums = sums + row_totals(value)
            squares = squares + row_totals(value * value)
        near_ref[t] = frames_ref[t, near]
        far_ref[t] = frames_ref[t, far]
        return sums, squares

    zero = jnp.zeros((8, channels), jnp.float32)
    sums, squares = lax.fori_loop(0, depth, step, (zero, zero))
    put_stats(out_ref, sums, squares)
    head_ref[...] = frames_ref[: depth - 2]
    last_ref[...] = frames_ref[depth - 2 :]


def pick_kernel(count, *refs):
    cell_refs, (near_ref, far_ref) = refs[:count], refs[-2:]
    near, far = sides(cell_refs[0].shape[1])
    t = 0
    for ref in cell_refs:
        for frame in range(ref.shape[0]):
            near_ref[t] = ref[frame, near]
            far_ref[t] = ref[frame, far]
            t += 1


def group_sum(value, size):
    channels = value.shape[1]
    lane = lax.broadcasted_iota(jnp.int32, value.shape, 1)
    step = 1
    while step < size:
        ahead = pltpu.roll(value, channels - step, 1)
        behind = pltpu.roll(value, step, 1)
        value = value + jnp.where((lane // step) % 2 == 0, ahead, behind)
        step *= 2
    return value


def scale_of(stats_ref, gain_ref, bias_ref, members):
    channels = stats_ref.shape[2]
    totals = jnp.sum(stats_ref[...], axis=0)
    totals = jnp.concatenate([totals, jnp.zeros((6, channels), jnp.float32)], axis=0)
    totals = group_sum(totals, channels // GROUPS)
    average = totals[0:1] / members
    spread = totals[1:2] / members - average * average
    factor = lax.rsqrt(spread + 1e-06) * gain_ref[...]
    return factor, bias_ref[...] - average * factor


def silu(value):
    return value * (0.5 * jnp.tanh(0.5 * value) + 0.5)


def edges(active_ref, scale):
    index, count = lax.axis_index("tile"), lax.axis_size("tile")
    height = active_ref.shape[1] - 2
    even = index % 2 == 0
    first = (lax.axis_index("tm") > 0).astype(jnp.float32)
    above = (index > 0).astype(jnp.float32)
    below = (index < count - 1).astype(jnp.float32)
    factor, offset = scale

    def put(t, h, value, keep):
        active = silu(value.astype(jnp.float32) * factor + offset)
        if keep is not None:
            active = active * keep
        active_ref[t, h] = active.astype(jnp.bfloat16)

    def fill(t, source):
        cells, near, far, is_past = source
        near, far = near[...], far[...]
        put(t, 0, jnp.where(even, far, near), above * first if is_past else above)
        for h in range(height):
            put(t, h + 1, cells[h], first if is_past else None)
        put(t, height + 1, jnp.where(even, near, far), below * first if is_past else below)

    return fill


def sources(pieces):
    found = []
    for cells, near, far, is_past in pieces:
        row = 0
        for ref in cells:
            for t in range(ref.shape[0]):
                found.append((ref.at[t], near.at[row], far.at[row], is_past))
                row += 1
    return found


def convolve(active_ref, weight_ref, t, height):
    columns, channels = active_ref.shape[2:]
    rows = height * columns
    totals = []
    for c in range(3):
        total = None
        for a in range(3):
            for b in range(3):
                piece = active_ref[t + a, b : b + height].reshape(rows, channels)
                part = jnp.dot(piece, weight_ref[a, b, c], preferred_element_type=jnp.float32)
                total = part if total is None else total + part
        totals.append(total)
    column = lax.broadcasted_iota(jnp.int32, totals[0].shape, 0) % columns
    left = jnp.where(column == 0, 0.0, pltpu.roll(totals[0], 1, 0))
    right = jnp.where(column == columns - 1, 0.0, pltpu.roll(totals[2], rows - 1, 0))
    return totals[1] + left + right


def split(refs, with_past):
    refs = list(refs)
    pieces = [((refs.pop(0),), refs.pop(0), refs.pop(0), True)] if with_past else []
    head, last, near, far = refs[:4]
    pieces.append(((head, last), near, far, False))
    return sources(pieces), refs[4:]


def first_kernel(members, begin, count, with_past, *refs):
    found, refs = split(refs, with_past)
    found = found if with_past else [None, None, *found]
    stats, gain, bias, weight = refs[:4]
    active_ref = refs[-1]
    height, columns, channels = active_ref.shape[1] - 2, *active_ref.shape[2:]
    even = lax.axis_index("tile") % 2 == 0
    fill = edges(active_ref, scale_of(stats, gain, bias, members))
    if begin == 0:
        totals, near_before, far_before, hidden_ref, totals_ref, near_ref, far_ref = refs[4:-1]
        near_ref[count:] = near_before[...]
        far_ref[count:] = far_before[...]
        sums, squares = totals[0], totals[1]
    else:
        hidden_ref, totals_ref, near_ref, far_ref = refs[4:-1]
        sums = squares = jnp.zeros((8, channels), jnp.float32)
    for t in range(2):
        fill(t, found[begin + t])
    for t in range(count):
        fill(t + 2, found[begin + t + 2])
        hidden = convolve(active_ref, weight, t, height).astype(jnp.bfloat16)
        wide = hidden.astype(jnp.float32)
        sums = sums + row_totals(wide)
        squares = squares + row_totals(wide * wide)
        hidden = hidden.reshape(height, columns, channels)
        hidden_ref[t] = hidden
        near_ref[t] = jnp.where(even, hidden[height - 1], hidden[0])
        far_ref[t] = jnp.where(even, hidden[0], hidden[height - 1])
    if begin == 0:
        put_stats(totals_ref, sums, squares)
    else:
        totals_ref[0] = sums
        totals_ref[1] = squares


def second_kernel(members, begin, count, with_past, *refs):
    found, refs = split(refs, with_past)
    found = found if with_past else [None, None, *found]
    stats, gain, bias, weight, frames, latent = refs[:6]
    active_ref, latents_ref, packed_ref, cells_ref, in_sem, out_sem = refs[-6:]
    height, columns, channels = active_ref.shape[1] - 2, *active_ref.shape[2:]
    parts, rows = packed_ref.shape[:2]
    if begin == 0:
        before, _, features_hbm, patches_ref = refs[6:-6]
        kept = rows - before.shape[1]
        packed_ref[:, kept:, :] = before[...].astype(jnp.float32)
    else:
        features_hbm, patches_ref = refs[6:-6]
        kept = rows
    loads = pltpu.make_async_copy(frames.at[begin : begin + count], cells_ref, in_sem)
    loads.start()
    width = LANES // 8
    pairs = height // 2
    blocks = kept // (count * pairs)
    lane = lax.broadcasted_iota(jnp.int32, (columns // 4, LANES), 1) // width
    spread = lax.broadcasted_iota(jnp.int32, (width, LANES), 0) == (
        lax.broadcasted_iota(jnp.int32, (width, LANES), 1) % width
    )
    wide_latent = lax.dot_general(
        latent[...], spread.astype(jnp.bfloat16), (((0,), (0,)), ((), ())),
        preferred_element_type=jnp.float32,
    ).astype(jnp.bfloat16)
    fill = edges(active_ref, scale_of(stats, gain, bias, members))
    for t in range(3):
        fill(t, found[begin + t])
    loads.wait()
    stores = []
    for t in range(count):
        if t > 0:
            fill(t + 2, found[begin + t + 2])
        branch = convolve(active_ref, weight, t, height)
        residual = cells_ref[t].reshape(height * columns, channels).astype(jnp.float32)
        features = (residual + branch).astype(jnp.bfloat16)
        cells_ref[t] = features.reshape(height, columns, channels)
        stores.append(
            pltpu.make_async_copy(cells_ref.at[t], features_hbm.at[begin + t], out_sem.at[t])
        )
        stores[-1].start()
        latents_ref[...] = (
            jnp.dot(features, wide_latent, preferred_element_type=jnp.float32)
            .astype(jnp.bfloat16)
            .astype(jnp.float32)
        )
        for i in range(pairs):
            mixed = None
            for cell in range(8):
                j, p, q = cell // 4, cell // 2 % 2, cell % 2
                start = (2 * i + p) * columns + 2 * j + q
                value = latents_ref[pl.ds(start, columns // 4, stride=4), :]
                mixed = value if mixed is None else jnp.where(lane == cell, value, mixed)
            for d in range(parts):
                packed_ref[d, pl.ds(t * blocks * pairs + i, blocks, stride=pairs), :] = mixed[
                    d * blocks : (d + 1) * blocks
                ]
    patches_ref[...] = packed_ref[...].astype(jnp.bfloat16)
    for store in stores:
        store.wait()


def unpack_kernel(blocks, pairs, received, tokens_ref, flat_ref, mixed_ref):
    parts, rows, lanes = received.shape
    flat_ref[...] = received[...].astype(jnp.float32).reshape(parts * rows, lanes)
    depth = rows // (blocks * pairs)
    for t in range(depth):
        for block in range(blocks):
            for i in range(pairs):
                start = (t * blocks + block) * pairs + i
                mixed_ref[t * blocks + block, pl.ds(i, parts, stride=pairs), :] = flat_ref[
                    pl.ds(start, parts, stride=rows), :
                ]
            tokens_ref[t, :, block * lanes : (block + 1) * lanes] = mixed_ref[
                t * blocks + block
            ].astype(jnp.bfloat16)


def sent_ahead(last):
    pairs = [(i, i + 1) for i in range(lax.axis_size("tm") - 1)]
    return lax.ppermute(last, "tm", pairs)


def sent_sideways(near, far):
    count = lax.axis_size("tile")
    near_pairs = [(i, i ^ 1) for i in range(count) if i ^ 1 < count]
    far_pairs = [pair for i in range(1, count - 1, 2) for pair in ((i, i + 1), (i + 1, i))]
    near = lax.ppermute(near, "tile", near_pairs)
    far = lax.ppermute(far, "tile", far_pairs)
    return near, far


def pick(cells, *after):
    rows = sum(piece.shape[0] for piece in cells)
    rows = jax.ShapeDtypeStruct((rows, *cells[0].shape[2:]), jnp.bfloat16)
    return pl.pallas_call(
        functools.partial(pick_kernel, len(cells)), out_shape=(rows, rows),
        in_specs=[VMEM] * len(cells) + [pl.BlockSpec(memory_space=pl.ANY)] * len(after),
        out_specs=(VMEM, VMEM), compiler_params=params(8), name="pick",
    )(*cells, *after)


def exchange(stats):
    return lax.all_to_all(stats, ALL, split_axis=0, concat_axis=0, tiled=True)


def body(frames, first_gain, first_bias, first_weight, second_gain, second_bias, second_weight,
         latent_weight):
    depth, height, columns, channels = frames.shape
    parts = lax.axis_size("tile")
    devices = lax.axis_size("tm") * parts
    members = float(devices * depth * height * columns * (channels // GROUPS))
    latent_width = latent_weight.shape[1]
    pairs = height // 2
    blocks = columns // 2 * 4 * latent_width // parts // LANES
    rows = depth * blocks * pairs
    stats_shape = jax.ShapeDtypeStruct((devices, 2, channels), jnp.float32)
    cells_shape = jax.ShapeDtypeStruct(frames.shape, jnp.bfloat16)
    last_shape = jax.ShapeDtypeStruct((2, *frames.shape[1:]), jnp.bfloat16)
    head_shape = jax.ShapeDtypeStruct((depth - 2, *frames.shape[1:]), jnp.bfloat16)

    row_shape = jax.ShapeDtypeStruct((depth, columns, channels), jnp.bfloat16)

    def active(count):
        return pltpu.VMEM((count + 2, height + 2, columns, channels), jnp.bfloat16)

    def cost(count):
        flops = 2 * 27 * count * height * columns * channels * channels
        return pl.CostEstimate(flops=flops, bytes_accessed=8 << 20, transcendentals=0)

    cells = pltpu.with_memory_space_constraint(frames, pltpu.HBM)
    stats, head, last, near, far = pl.pallas_call(
        stats_kernel, out_shape=(stats_shape, head_shape, last_shape, row_shape, row_shape),
        in_specs=[VMEM], out_specs=(VMEM,) * 5, compiler_params=params(8), cost_estimate=cost(1),
        name="stats",
    )(frames)

    def gather(near, far, last, stats):
        past = sent_ahead(last)
        near, far = sent_sideways(near, far)
        stats = exchange(stats)
        corner = sent_sideways(*pick((past,), stats))
        return (past, *corner), near, far, stats

    alone = depth >= 4
    ahead_shape = jax.ShapeDtypeStruct((2, columns, channels), jnp.bfloat16)
    around, near, far, stats = gather(near, far, last, stats)
    own = (head, last, near, far, stats, first_gain[None], first_bias[None], first_weight)
    ahead = (() if alone else around) + own
    last, totals, near, far = pl.pallas_call(
        functools.partial(first_kernel, members, depth - 2, 2, not alone),
        out_shape=(last_shape, jax.ShapeDtypeStruct((2, 8, channels), jnp.float32),
                   ahead_shape, ahead_shape),
        in_specs=[VMEM] * len(ahead), out_specs=(VMEM,) * 4, scratch_shapes=[active(2)],
        compiler_params=params(24), cost_estimate=cost(2), name="first_last",
    )(*ahead)
    head, stats, near, far = pl.pallas_call(
        functools.partial(first_kernel, members, 0, depth - 2, True),
        out_shape=(head_shape, stats_shape, row_shape, row_shape),
        in_specs=[VMEM] * 14, out_specs=(VMEM,) * 4, scratch_shapes=[active(depth - 2)],
        compiler_params=params(24), cost_estimate=cost(depth - 2), name="first_head",
    )(*around, *own, totals, near, far)

    tail_rows = 2 * blocks * pairs

    def scratch(count, held):
        return [
            active(count), pltpu.VMEM((height * columns, LANES), jnp.float32),
            pltpu.VMEM((parts, held, LANES), jnp.float32),
            pltpu.VMEM((count, *frames.shape[1:]), jnp.bfloat16),
            pltpu.SemaphoreType.DMA(()), pltpu.SemaphoreType.DMA((count,)),
        ]

    around, near, far, stats = gather(near, far, last, stats)
    own = (head, last, near, far, stats, second_gain[None], second_bias[None], second_weight,
           cells, latent_weight.T)
    ahead = (() if alone else around) + own
    features, patches = pl.pallas_call(
        functools.partial(second_kernel, members, depth - 2, 2, not alone),
        out_shape=(cells_shape,
                   jax.ShapeDtypeStruct((parts, tail_rows, LANES), jnp.bfloat16)),
        in_specs=[VMEM] * (len(ahead) - 2) + [HBM, VMEM], out_specs=(HBM, VMEM),
        scratch_shapes=scratch(2, tail_rows),
        compiler_params=params(24), cost_estimate=cost(2), name="second_last",
    )(*ahead)
    features, patches = pl.pallas_call(
        functools.partial(second_kernel, members, 0, depth - 2, True),
        out_shape=(cells_shape, jax.ShapeDtypeStruct((parts, rows, LANES), jnp.bfloat16)),
        in_specs=[VMEM] * 11 + [HBM, VMEM, VMEM, HBM], out_specs=(HBM, VMEM),
        scratch_shapes=scratch(depth - 2, rows), input_output_aliases={14: 0},
        compiler_params=params(24), cost_estimate=cost(depth - 2), name="second_head",
    )(*around, *own, patches, features)
    received = lax.all_to_all(patches, "tile", split_axis=0, concat_axis=0, tiled=True)
    tokens = pl.pallas_call(
        functools.partial(unpack_kernel, blocks, pairs),
        out_shape=jax.ShapeDtypeStruct((depth, parts * pairs, blocks * LANES), jnp.bfloat16),
        in_specs=[VMEM], out_specs=VMEM,
        scratch_shapes=[pltpu.VMEM((parts * rows, LANES), jnp.float32),
                        pltpu.VMEM((depth * blocks, parts * pairs, LANES), jnp.float32)],
        compiler_params=params(16), name="unpack",
    )(received)
    return features, tokens


def solution(mesh):
    in_specs = (P("tm", "tile", None, None), P(), P(), P(), P(), P(), P(), P())
    out_specs = (P("tm", "tile", None, None), P("tm", None, "tile"))
    return jax.shard_map(body, mesh=mesh, in_specs=in_specs, out_specs=out_specs, check_vma=False)
```

```python
import functools

import jax
import jax.numpy as jnp
from jax import lax
from jax.experimental import pallas as pl
from jax.experimental.pallas import tpu as pltpu
from jax.sharding import PartitionSpec as P


GROUPS = 32
ALL = ("tm", "tile")
VMEM = pl.BlockSpec(memory_space=pltpu.VMEM)
HBM = pl.BlockSpec(memory_space=pltpu.HBM)
LANES = 128


def params(mib):
    return pltpu.CompilerParams(vmem_limit_bytes=mib << 20)


def row_totals(value):
    folded = value.reshape(-1, 8, value.shape[-1])
    return jnp.sum(folded, axis=0)


def put_stats(out_ref, sums, squares):
    pair = jnp.concatenate(
        [jnp.sum(sums, axis=0, keepdims=True), jnp.sum(squares, axis=0, keepdims=True)], axis=0
    )
    out_ref[...] = jnp.broadcast_to(pair[None], out_ref.shape)


def sides(height):
    even = lax.axis_index("tile") % 2 == 0
    return jnp.where(even, height - 1, 0), jnp.where(even, 0, height - 1)


def stats_kernel(frames_ref, out_ref, head_ref, last_ref):
    depth, height, _, channels = frames_ref.shape

    def step(t, carry):
        sums, squares = carry
        for h in range(height):
            value = frames_ref[t, h].astype(jnp.float32)
            sums = sums + row_totals(value)
            squares = squares + row_totals(value * value)
        return sums, squares

    zero = jnp.zeros((8, channels), jnp.float32)
    sums, squares = lax.fori_loop(0, depth, step, (zero, zero))
    put_stats(out_ref, sums, squares)
    head_ref[...] = frames_ref[: depth - 2]
    last_ref[...] = frames_ref[depth - 2 :]


def pick_kernel(count, *refs):
    cell_refs, (near_ref, far_ref) = refs[:count], refs[-2:]
    near, far = sides(cell_refs[0].shape[1])
    t = 0
    for ref in cell_refs:
        for frame in range(ref.shape[0]):
            near_ref[t] = ref[frame, near]
            far_ref[t] = ref[frame, far]
            t += 1


def group_sum(value, size):
    channels = value.shape[1]
    lane = lax.broadcasted_iota(jnp.int32, value.shape, 1)
    step = 1
    while step < size:
        ahead = pltpu.roll(value, channels - step, 1)
        behind = pltpu.roll(value, step, 1)
        value = value + jnp.where((lane // step) % 2 == 0, ahead, behind)
        step *= 2
    return value


def scale_of(stats_ref, gain_ref, bias_ref, members):
    channels = stats_ref.shape[2]
    totals = jnp.sum(stats_ref[...], axis=0)
    totals = jnp.concatenate([totals, jnp.zeros((6, channels), jnp.float32)], axis=0)
    totals = group_sum(totals, channels // GROUPS)
    average = totals[0:1] / members
    spread = totals[1:2] / members - average * average
    factor = lax.rsqrt(spread + 1e-06) * gain_ref[...]
    return factor, bias_ref[...] - average * factor


def silu(value):
    return value * (0.5 * jnp.tanh(0.5 * value) + 0.5)


def activate(value, scale, keep):
    factor, offset = scale
    active = silu(value.astype(jnp.float32) * factor + offset)
    if keep is not None:
        active = active * keep
    return active.astype(jnp.bfloat16)


def has_past():
    return (lax.axis_index("tm") > 0).astype(jnp.float32)


def convolve(piece, weight_ref, columns):
    totals = []
    for c in range(3):
        total = None
        for a in range(3):
            for b in range(3):
                part = jnp.dot(piece(a, b), weight_ref[a, b, c], preferred_element_type=jnp.float32)
                total = part if total is None else total + part
        totals.append(total)
    rows = totals[0].shape[0]
    column = lax.broadcasted_iota(jnp.int32, totals[0].shape, 0) % columns
    left = jnp.where(column == 0, 0.0, pltpu.roll(totals[0], 1, 0))
    right = jnp.where(column == columns - 1, 0.0, pltpu.roll(totals[2], rows - 1, 0))
    return totals[1] + left + right


def steps(count):
    return [(t, min(2, count - t)) for t in range(0, count, 2)]


def inner(members, past, head, last, stats, gain, bias, weight, active_ref, finish):
    height, columns, channels = active_ref.shape[1:]
    scale = scale_of(stats, gain, bias, members)
    first = has_past()
    found = [(ref.at[t], ref is past) for ref in (past, head, last) for t in range(ref.shape[0])]
    done = 0
    for t, count in steps(len(found) - 2):
        while done < t + count + 2:
            cells, is_past = found[done]
            for h in range(height):
                active_ref[done, h] = activate(cells[h], scale, first if is_past else None)
            done += 1

        def piece(a, b, t=t, count=count):
            cells = active_ref[t + a : t + a + count, b : b + height - 2]
            return cells.reshape(count * (height - 2) * columns, channels)

        finish(t, count, convolve(piece, weight, columns))


def inner_first(members, past, head, last, stats, gain, bias, weight,
                active_ref, inner_ref, totals_ref):
    totals_ref[...] = jnp.zeros_like(totals_ref)

    def finish(t, count, total):
        hidden = total.astype(jnp.bfloat16)
        inner_ref[t : t + count] = hidden.reshape(count, *inner_ref.shape[1:])
        wide = hidden.astype(jnp.float32)
        totals_ref[0] += row_totals(wide)
        totals_ref[1] += row_totals(wide * wide)

    inner(members, past, head, last, stats, gain, bias, weight, active_ref, finish)


def inner_second(members, past, head, last, stats, gain, bias, weight, frames,
                 active_ref, inner_ref, cells_ref, sem):
    height = frames.shape[1]
    loads = pltpu.make_async_copy(frames.at[:, 1 : height - 1], cells_ref, sem)
    loads.start()
    loads.wait()

    def finish(t, count, total):
        cells = cells_ref[t : t + count].astype(jnp.float32).reshape(total.shape)
        inner_ref[t : t + count] = (cells + total).astype(jnp.bfloat16).reshape(
            count, *inner_ref.shape[1:]
        )

    inner(members, past, head, last, stats, gain, bias, weight, active_ref, finish)


def outer(members, begin, frames, near, far, active, stats, gain, bias, weight, halo_ref, finish):
    height, columns = active.shape[1:3]
    scale = scale_of(stats, gain, bias, members)
    index, count = lax.axis_index("tile"), lax.axis_size("tile")
    even = index % 2 == 0
    first = has_past()
    above = (index > 0).astype(jnp.float32)
    below = (index < count - 1).astype(jnp.float32)
    for t in range(frames + 2):
        e = begin + t
        rows = near[e], far[e]
        top, bottom = (above * first, below * first) if e < 2 else (above, below)
        halo_ref[t, 0] = activate(jnp.where(even, rows[1], rows[0]), scale, top)
        halo_ref[t, 1] = activate(jnp.where(even, rows[0], rows[1]), scale, bottom)

    def row(t, h):
        if h == 0:
            return halo_ref[t, 0]
        if h == height + 1:
            return halo_ref[t, 1]
        return active[begin + t, h - 1]

    for t, count in steps(frames):

        def piece(a, b, t=t, count=count):
            cells = [
                row(t + a + f, h + b) for f in range(count) for h in (0, height - 1)
            ]
            return jnp.concatenate(cells, axis=0)

        finish(t, count, convolve(piece, weight, columns))


def outer_first(members, begin, frames, near, far, active, stats, gain, bias, weight, inside,
                before, cells_ref, totals_ref, halo_ref):
    height, columns, channels = cells_ref.shape[1:]
    sums, squares = [before[0]], [before[1]]

    def finish(t, count, total):
        hidden = total.astype(jnp.bfloat16)
        rows = hidden.reshape(count, 2, columns, channels)
        for f in range(count):
            cells_ref[t + f, 0] = rows[f, 0]
            cells_ref[t + f, height - 1] = rows[f, 1]
        wide = hidden.astype(jnp.float32)
        sums.append(row_totals(wide))
        squares.append(row_totals(wide * wide))

    cells_ref[:, 1 : height - 1] = inside[begin : begin + frames]
    outer(members, begin, frames, near, far, active, stats, gain, bias, weight, halo_ref, finish)
    if begin == 0:
        put_stats(totals_ref, sum(sums), sum(squares))
    else:
        totals_ref[0] = sum(sums)
        totals_ref[1] = sum(squares)


def outer_second(members, near, far, active, stats, gain, bias, weight, inside, frames, latent,
                 features_hbm, patches_ref, halo_ref, cells_ref, latents_ref, packed_ref, sem):
    depth, height, columns, channels = cells_ref.shape
    loads = [
        pltpu.make_async_copy(frames.at[:, h : h + 1], cells_ref.at[:, h : h + 1], sem.at[n])
        for n, h in enumerate((0, height - 1))
    ]
    for load in loads:
        load.start()
    width = LANES // 8
    parts, rows = packed_ref.shape[:2]
    pairs = height // 2
    blocks = rows // (depth * pairs)
    lane = lax.broadcasted_iota(jnp.int32, (columns // 4, LANES), 1) // width
    spread = lax.broadcasted_iota(jnp.int32, (width, LANES), 0) == (
        lax.broadcasted_iota(jnp.int32, (width, LANES), 1) % width
    )
    wide_latent = lax.dot_general(
        latent[...], spread.astype(jnp.bfloat16), (((0,), (0,)), ((), ())),
        preferred_element_type=jnp.float32,
    ).astype(jnp.bfloat16)
    for load in loads:
        load.wait()
    cells_ref[:, 1 : height - 1] = inside[...]

    def finish(t, count, total):
        branch = total.reshape(count, 2, columns, channels)
        for f in range(count):
            for n, h in enumerate((0, height - 1)):
                cells = cells_ref[t + f, h].astype(jnp.float32)
                cells_ref[t + f, h] = (cells + branch[f, n]).astype(jnp.bfloat16)

    outer(members, 0, depth, near, far, active, stats, gain, bias, weight, halo_ref, finish)
    store = pltpu.make_async_copy(cells_ref, features_hbm, sem.at[2])
    store.start()

    def step(t, carry):
        latents_ref[...] = (
            jnp.dot(
                cells_ref[t].reshape(height * columns, channels), wide_latent,
                preferred_element_type=jnp.float32,
            )
            .astype(jnp.bfloat16)
            .astype(jnp.float32)
        )
        for i in range(pairs):
            mixed = None
            for cell in range(8):
                j, p, q = cell // 4, cell // 2 % 2, cell % 2
                start = (2 * i + p) * columns + 2 * j + q
                value = latents_ref[pl.ds(start, columns // 4, stride=4), :]
                mixed = value if mixed is None else jnp.where(lane == cell, value, mixed)
            for d in range(parts):
                packed_ref[d, pl.ds(t * blocks * pairs + i, blocks, stride=pairs), :] = mixed[
                    d * blocks : (d + 1) * blocks
                ]
        return carry

    lax.fori_loop(0, depth, step, 0)
    patches_ref[...] = packed_ref[...].astype(jnp.bfloat16)
    store.wait()


def unpack_kernel(blocks, pairs, received, tokens_ref, flat_ref, mixed_ref):
    parts, rows, lanes = received.shape
    flat_ref[...] = received[...].astype(jnp.float32).reshape(parts * rows, lanes)
    depth = rows // (blocks * pairs)
    for t in range(depth):
        for block in range(blocks):
            for i in range(pairs):
                start = (t * blocks + block) * pairs + i
                mixed_ref[t * blocks + block, pl.ds(i, parts, stride=pairs), :] = flat_ref[
                    pl.ds(start, parts, stride=rows), :
                ]
            tokens_ref[t, :, block * lanes : (block + 1) * lanes] = mixed_ref[
                t * blocks + block
            ].astype(jnp.bfloat16)


def sent_ahead(last):
    pairs = [(i, i + 1) for i in range(lax.axis_size("tm") - 1)]
    return lax.ppermute(last, "tm", pairs)


def sent_sideways(near, far):
    count = lax.axis_size("tile")
    near_pairs = [(i, i ^ 1) for i in range(count) if i ^ 1 < count]
    far_pairs = [pair for i in range(1, count - 1, 2) for pair in ((i, i + 1), (i + 1, i))]
    near = lax.ppermute(near, "tile", near_pairs)
    far = lax.ppermute(far, "tile", far_pairs)
    return near, far


def pick(cells, *after):
    rows = sum(piece.shape[0] for piece in cells)
    rows = jax.ShapeDtypeStruct((rows, *cells[0].shape[2:]), jnp.bfloat16)
    return pl.pallas_call(
        functools.partial(pick_kernel, len(cells)), out_shape=(rows, rows),
        in_specs=[VMEM] * len(cells) + [pl.BlockSpec(memory_space=pl.ANY)] * len(after),
        out_specs=(VMEM, VMEM), compiler_params=params(8), name="pick",
    )(*cells, *after)


def exchange(stats):
    return lax.all_to_all(stats, ALL, split_axis=0, concat_axis=0, tiled=True)


def body(frames, first_gain, first_bias, first_weight, second_gain, second_bias, second_weight,
         latent_weight):
    depth, height, columns, channels = frames.shape
    parts = lax.axis_size("tile")
    devices = lax.axis_size("tm") * parts
    members = float(devices * depth * height * columns * (channels // GROUPS))
    latent_width = latent_weight.shape[1]
    pairs = height // 2
    blocks = columns // 2 * 4 * latent_width // parts // LANES
    rows = depth * blocks * pairs
    stats_shape = jax.ShapeDtypeStruct((devices, 2, channels), jnp.float32)
    cells_shape = jax.ShapeDtypeStruct(frames.shape, jnp.bfloat16)
    last_shape = jax.ShapeDtypeStruct((2, *frames.shape[1:]), jnp.bfloat16)
    head_shape = jax.ShapeDtypeStruct((depth - 2, *frames.shape[1:]), jnp.bfloat16)

    active_shape = jax.ShapeDtypeStruct((depth + 2, height, columns, channels), jnp.bfloat16)
    inner_shape = jax.ShapeDtypeStruct((depth, height - 2, columns, channels), jnp.bfloat16)
    totals_shape = jax.ShapeDtypeStruct((2, 8, channels), jnp.float32)

    def halo(count):
        return pltpu.VMEM((count + 2, 2, columns, channels), jnp.bfloat16)

    def call(kernel, outs, inputs, count, scratch=(), hbm=(), out_specs=None):
        flops = 27 * count * height * columns * channels * channels
        return pl.pallas_call(
            kernel, out_shape=outs, in_specs=[HBM if i in hbm else VMEM for i in range(len(inputs))],
            out_specs=out_specs or (VMEM,) * len(outs), scratch_shapes=list(scratch),
            compiler_params=params(24),
            cost_estimate=pl.CostEstimate(flops=flops, bytes_accessed=8 << 20, transcendentals=0),
        )(*inputs)

    def gather(head, last, stats):
        past = sent_ahead(last)
        stats = exchange(stats)
        near, far = sent_sideways(*pick((past, head, last), stats))
        return past, near, far, stats

    cells = pltpu.with_memory_space_constraint(frames, pltpu.HBM)
    stats, head, last = call(stats_kernel, (stats_shape, head_shape, last_shape), (frames,), 2)
    past, near, far, stats = gather(head, last, stats)
    norm = (stats, first_gain[None], first_bias[None], first_weight)
    active, inside, totals = call(
        functools.partial(inner_first, members),
        (active_shape, inner_shape, totals_shape), (past, head, last, *norm), depth,
    )
    around = (near, far, active, *norm, inside)
    last, totals = call(
        functools.partial(outer_first, members, depth - 2, 2),
        (last_shape, totals_shape), (*around, totals), 2, (halo(2),),
    )
    head, stats = call(
        functools.partial(outer_first, members, 0, depth - 2),
        (head_shape, stats_shape), (*around, totals), depth - 2, (halo(depth - 2),),
    )
    past, near, far, stats = gather(head, last, stats)
    norm = (stats, second_gain[None], second_bias[None], second_weight)
    active, inside = call(
        functools.partial(inner_second, members),
        (active_shape, inner_shape), (past, head, last, *norm, cells), depth,
        (pltpu.VMEM(inner_shape.shape, jnp.bfloat16), pltpu.SemaphoreType.DMA(())), (7,),
    )
    features, patches = call(
        functools.partial(outer_second, members),
        (cells_shape, jax.ShapeDtypeStruct((parts, rows, LANES), jnp.bfloat16)),
        (near, far, active, *norm, inside, cells, latent_weight.T), depth,
        (halo(depth), pltpu.VMEM(frames.shape, jnp.bfloat16),
         pltpu.VMEM((height * columns, LANES), jnp.float32),
         pltpu.VMEM((parts, rows, LANES), jnp.float32), pltpu.SemaphoreType.DMA((3,))),
        (8,), (HBM, VMEM),
    )
    received = lax.all_to_all(patches, "tile", split_axis=0, concat_axis=0, tiled=True)
    tokens = pl.pallas_call(
        functools.partial(unpack_kernel, blocks, pairs),
        out_shape=jax.ShapeDtypeStruct((depth, parts * pairs, blocks * LANES), jnp.bfloat16),
        in_specs=[VMEM], out_specs=VMEM,
        scratch_shapes=[pltpu.VMEM((parts * rows, LANES), jnp.float32),
                        pltpu.VMEM((depth * blocks, parts * pairs, LANES), jnp.float32)],
        compiler_params=params(16), name="unpack",
    )(received)
    return features, tokens


def solution(mesh):
    in_specs = (P("tm", "tile", None, None), P(), P(), P(), P(), P(), P(), P())
    out_specs = (P("tm", "tile", None, None), P("tm", None, "tile"))
    return jax.shard_map(body, mesh=mesh, in_specs=in_specs, out_specs=out_specs, check_vma=False)
```

```python
import functools

import jax
import jax.numpy as jnp
from jax import lax
from jax.experimental import pallas as pl
from jax.experimental.pallas import tpu as pltpu
from jax.sharding import PartitionSpec as P


GROUPS = 32
ALL = ("tm", "tile")
VMEM = pl.BlockSpec(memory_space=pltpu.VMEM)
HBM = pl.BlockSpec(memory_space=pltpu.HBM)
LANES = 128


def params(mib):
    return pltpu.CompilerParams(vmem_limit_bytes=mib << 20)


def row_totals(value):
    folded = value.reshape(-1, 8, value.shape[-1])
    return jnp.sum(folded, axis=0)


def put_stats(out_ref, sums, squares):
    pair = jnp.concatenate(
        [jnp.sum(sums, axis=0, keepdims=True), jnp.sum(squares, axis=0, keepdims=True)], axis=0
    )
    out_ref[...] = jnp.broadcast_to(pair[None], out_ref.shape)


def sides(height):
    even = lax.axis_index("tile") % 2 == 0
    return jnp.where(even, height - 1, 0), jnp.where(even, 0, height - 1)


def stats_kernel(frames_ref, out_ref, head_ref, last_ref, near_ref, far_ref):
    depth, height, _, channels = frames_ref.shape
    near, far = sides(height)

    def step(t, carry):
        sums, squares = carry
        for h in range(height):
            value = frames_ref[t, h].astype(jnp.float32)
            sums = sums + row_totals(value)
            squares = squares + row_totals(value * value)
        near_ref[t] = frames_ref[t, near]
        far_ref[t] = frames_ref[t, far]
        return sums, squares

    zero = jnp.zeros((8, channels), jnp.float32)
    sums, squares = lax.fori_loop(0, depth, step, (zero, zero))
    put_stats(out_ref, sums, squares)
    head_ref[...] = frames_ref[: depth - 2]
    last_ref[...] = frames_ref[depth - 2 :]


def pick_kernel(count, *refs):
    cell_refs, (near_ref, far_ref) = refs[:count], refs[-2:]
    near, far = sides(cell_refs[0].shape[1])
    t = 0
    for ref in cell_refs:
        for frame in range(ref.shape[0]):
            near_ref[t] = ref[frame, near]
            far_ref[t] = ref[frame, far]
            t += 1


def group_sum(value, size):
    channels = value.shape[1]
    lane = lax.broadcasted_iota(jnp.int32, value.shape, 1)
    step = 1
    while step < size:
        ahead = pltpu.roll(value, channels - step, 1)
        behind = pltpu.roll(value, step, 1)
        value = value + jnp.where((lane // step) % 2 == 0, ahead, behind)
        step *= 2
    return value


def scale_of(stats_ref, gain_ref, bias_ref, members):
    channels = stats_ref.shape[2]
    totals = jnp.sum(stats_ref[...], axis=0)
    totals = jnp.concatenate([totals, jnp.zeros((6, channels), jnp.float32)], axis=0)
    totals = group_sum(totals, channels // GROUPS)
    average = totals[0:1] / members
    spread = totals[1:2] / members - average * average
    factor = lax.rsqrt(spread + 1e-06) * gain_ref[...]
    return factor, bias_ref[...] - average * factor


def silu(value):
    return value * (0.5 * jnp.tanh(0.5 * value) + 0.5)


def activate(value, scale, keep):
    factor, offset = scale
    active = silu(value.astype(jnp.float32) * factor + offset)
    if keep is not None:
        active = active * keep
    return active.astype(jnp.bfloat16)


def has_past():
    return (lax.axis_index("tm") > 0).astype(jnp.float32)


def convolve(piece, weight_ref, columns):
    totals = []
    for c in range(3):
        total = None
        for a in range(3):
            for b in range(3):
                part = jnp.dot(piece(a, b), weight_ref[a, b, c], preferred_element_type=jnp.float32)
                total = part if total is None else total + part
        totals.append(total)
    rows = totals[0].shape[0]
    column = lax.broadcasted_iota(jnp.int32, totals[0].shape, 0) % columns
    left = jnp.where(column == 0, 0.0, pltpu.roll(totals[0], 1, 0))
    right = jnp.where(column == columns - 1, 0.0, pltpu.roll(totals[2], rows - 1, 0))
    return totals[1] + left + right


def steps(count):
    return [(t, min(2, count - t)) for t in range(0, count, 2)]


def edges(active_ref, scale):
    index, count = lax.axis_index("tile"), lax.axis_size("tile")
    height = active_ref.shape[1] - 2
    even = index % 2 == 0
    first = (lax.axis_index("tm") > 0).astype(jnp.float32)
    above = (index > 0).astype(jnp.float32)
    below = (index < count - 1).astype(jnp.float32)
    factor, offset = scale

    def put(t, h, value, keep):
        active = silu(value.astype(jnp.float32) * factor + offset)
        if keep is not None:
            active = active * keep
        active_ref[t, h] = active.astype(jnp.bfloat16)

    def fill(t, source):
        cells, near, far, is_past = source
        near, far = near[...], far[...]
        put(t, 0, jnp.where(even, far, near), above * first if is_past else above)
        for h in range(height):
            put(t, h + 1, cells[h], first if is_past else None)
        put(t, height + 1, jnp.where(even, near, far), below * first if is_past else below)

    return fill


def sources(pieces):
    found = []
    for cells, near, far, is_past in pieces:
        row = 0
        for ref in cells:
            for t in range(ref.shape[0]):
                found.append((ref.at[t], near.at[row], far.at[row], is_past))
                row += 1
    return found


def split(refs, with_past):
    refs = list(refs)
    pieces = [((refs.pop(0),), refs.pop(0), refs.pop(0), True)] if with_past else []
    head, last, near, far = refs[:4]
    pieces.append(((head, last), near, far, False))
    return sources(pieces), refs[4:]


def first_kernel(members, begin, count, with_past, *refs):
    found, refs = split(refs, with_past)
    found = found if with_past else [None, None, *found]
    stats, gain, bias, weight = refs[:4]
    active_ref = refs[-1]
    height, columns, channels = active_ref.shape[1] - 2, *active_ref.shape[2:]
    fill = edges(active_ref, scale_of(stats, gain, bias, members))
    if begin == 0:
        totals, hidden_ref, totals_ref = refs[4:-1]
        sums, squares = totals[0], totals[1]
    else:
        hidden_ref, totals_ref = refs[4:-1]
        sums = squares = jnp.zeros((8, channels), jnp.float32)
    for t in range(2):
        fill(t, found[begin + t])
    for t in range(count):
        fill(t + 2, found[begin + t + 2])

        def piece(a, b, t=t):
            return active_ref[t + a, b : b + height].reshape(height * columns, channels)

        hidden = convolve(piece, weight, columns).astype(jnp.bfloat16)
        wide = hidden.astype(jnp.float32)
        sums = sums + row_totals(wide)
        squares = squares + row_totals(wide * wide)
        hidden_ref[t] = hidden.reshape(height, columns, channels)
    if begin == 0:
        put_stats(totals_ref, sums, squares)
    else:
        totals_ref[0] = sums
        totals_ref[1] = squares


def inner(members, past, head, last, stats, gain, bias, weight, active_ref, finish):
    height, columns, channels = active_ref.shape[1:]
    scale = scale_of(stats, gain, bias, members)
    first = has_past()
    found = [(ref.at[t], ref is past) for ref in (past, head, last) for t in range(ref.shape[0])]
    done = 0
    for t, count in steps(len(found) - 2):
        while done < t + count + 2:
            cells, is_past = found[done]
            for h in range(height):
                active_ref[done, h] = activate(cells[h], scale, first if is_past else None)
            done += 1

        def piece(a, b, t=t, count=count):
            cells = active_ref[t + a : t + a + count, b : b + height - 2]
            return cells.reshape(count * (height - 2) * columns, channels)

        finish(t, count, convolve(piece, weight, columns))


def inner_second(members, past, head, last, stats, gain, bias, weight, frames,
                 active_ref, inner_ref):
    height = frames.shape[1]

    def finish(t, count, total):
        cells = frames[t : t + count, 1 : height - 1].astype(jnp.float32).reshape(total.shape)
        inner_ref[t : t + count] = (cells + total).astype(jnp.bfloat16).reshape(
            count, *inner_ref.shape[1:]
        )

    inner(members, past, head, last, stats, gain, bias, weight, active_ref, finish)


def outer(members, begin, frames, near, far, active, stats, gain, bias, weight, halo_ref, finish):
    height, columns = active.shape[1:3]
    scale = scale_of(stats, gain, bias, members)
    index, count = lax.axis_index("tile"), lax.axis_size("tile")
    even = index % 2 == 0
    first = has_past()
    above = (index > 0).astype(jnp.float32)
    below = (index < count - 1).astype(jnp.float32)
    for t in range(frames + 2):
        e = begin + t
        rows = near[e], far[e]
        top, bottom = (above * first, below * first) if e < 2 else (above, below)
        halo_ref[t, 0] = activate(jnp.where(even, rows[1], rows[0]), scale, top)
        halo_ref[t, 1] = activate(jnp.where(even, rows[0], rows[1]), scale, bottom)

    def row(t, h):
        if h == 0:
            return halo_ref[t, 0]
        if h == height + 1:
            return halo_ref[t, 1]
        return active[begin + t, h - 1]

    for t, count in steps(frames):

        def piece(a, b, t=t, count=count):
            cells = [
                row(t + a + f, h + b) for f in range(count) for h in (0, height - 1)
            ]
            return jnp.concatenate(cells, axis=0)

        finish(t, count, convolve(piece, weight, columns))


def outer_second(members, near, far, active, stats, gain, bias, weight, inside, frames, latent,
                 features_hbm, patches_ref, halo_ref, cells_ref, latents_ref, packed_ref, sem):
    depth, height, columns, channels = cells_ref.shape
    stores = [pltpu.make_async_copy(inside, features_hbm.at[:, 1 : height - 1], sem.at[2])]
    stores[0].start()
    width = LANES // 8
    parts, rows = packed_ref.shape[:2]
    pairs = height // 2
    blocks = rows // (depth * pairs)
    lane = lax.broadcasted_iota(jnp.int32, (columns // 4, LANES), 1) // width
    spread = lax.broadcasted_iota(jnp.int32, (width, LANES), 0) == (
        lax.broadcasted_iota(jnp.int32, (width, LANES), 1) % width
    )
    wide_latent = lax.dot_general(
        latent[...], spread.astype(jnp.bfloat16), (((0,), (0,)), ((), ())),
        preferred_element_type=jnp.float32,
    ).astype(jnp.bfloat16)
    cells_ref[:, 1 : height - 1] = inside[...]

    def finish(t, count, total):
        branch = total.reshape(count, 2, columns, channels)
        for f in range(count):
            for n, h in enumerate((0, height - 1)):
                cells = frames[t + f, h].astype(jnp.float32)
                cells_ref[t + f, h] = (cells + branch[f, n]).astype(jnp.bfloat16)

    outer(members, 0, depth, near, far, active, stats, gain, bias, weight, halo_ref, finish)
    for n, h in enumerate((0, height - 1)):
        stores.append(
            pltpu.make_async_copy(
                cells_ref.at[:, h : h + 1], features_hbm.at[:, h : h + 1], sem.at[n]
            )
        )
        stores[-1].start()
    for t in range(depth):
        latents_ref[t] = (
            jnp.dot(
                cells_ref[t].reshape(height * columns, channels), wide_latent,
                preferred_element_type=jnp.float32,
            )
            .astype(jnp.bfloat16)
            .astype(jnp.float32)
        )
    for t in range(depth):
        for i in range(pairs):
            mixed = None
            for cell in range(8):
                j, p, q = cell // 4, cell // 2 % 2, cell % 2
                start = (2 * i + p) * columns + 2 * j + q
                value = latents_ref[t, pl.ds(start, columns // 4, stride=4), :]
                mixed = value if mixed is None else jnp.where(lane == cell, value, mixed)
            for d in range(parts):
                packed_ref[d, pl.ds(t * blocks * pairs + i, blocks, stride=pairs), :] = mixed[
                    d * blocks : (d + 1) * blocks
                ]
    patches_ref[...] = packed_ref[...].astype(jnp.bfloat16)
    for store in stores:
        store.wait()


def unpack_kernel(blocks, pairs, received, tokens_ref, flat_ref, mixed_ref):
    parts, rows, lanes = received.shape
    flat_ref[...] = received[...].astype(jnp.float32).reshape(parts * rows, lanes)
    depth = rows // (blocks * pairs)
    for t in range(depth):
        for block in range(blocks):
            for i in range(pairs):
                start = (t * blocks + block) * pairs + i
                mixed_ref[t * blocks + block, pl.ds(i, parts, stride=pairs), :] = flat_ref[
                    pl.ds(start, parts, stride=rows), :
                ]
            tokens_ref[t, :, block * lanes : (block + 1) * lanes] = mixed_ref[
                t * blocks + block
            ].astype(jnp.bfloat16)


def sent_ahead(last):
    pairs = [(i, i + 1) for i in range(lax.axis_size("tm") - 1)]
    return lax.ppermute(last, "tm", pairs)


def sent_sideways(near, far):
    count = lax.axis_size("tile")
    near_pairs = [(i, i ^ 1) for i in range(count) if i ^ 1 < count]
    far_pairs = [pair for i in range(1, count - 1, 2) for pair in ((i, i + 1), (i + 1, i))]
    near = lax.ppermute(near, "tile", near_pairs)
    far = lax.ppermute(far, "tile", far_pairs)
    return near, far


def pick(cells, *after):
    rows = sum(piece.shape[0] for piece in cells)
    rows = jax.ShapeDtypeStruct((rows, *cells[0].shape[2:]), jnp.bfloat16)
    return pl.pallas_call(
        functools.partial(pick_kernel, len(cells)), out_shape=(rows, rows),
        in_specs=[VMEM] * len(cells) + [pl.BlockSpec(memory_space=pl.ANY)] * len(after),
        out_specs=(VMEM, VMEM), compiler_params=params(8), name="pick",
    )(*cells, *after)


def exchange(stats):
    return lax.all_to_all(stats, ALL, split_axis=0, concat_axis=0, tiled=True)


def body(frames, first_gain, first_bias, first_weight, second_gain, second_bias, second_weight,
         latent_weight):
    depth, height, columns, channels = frames.shape
    parts = lax.axis_size("tile")
    devices = lax.axis_size("tm") * parts
    members = float(devices * depth * height * columns * (channels // GROUPS))
    latent_width = latent_weight.shape[1]
    pairs = height // 2
    blocks = columns // 2 * 4 * latent_width // parts // LANES
    rows = depth * blocks * pairs
    stats_shape = jax.ShapeDtypeStruct((devices, 2, channels), jnp.float32)
    cells_shape = jax.ShapeDtypeStruct(frames.shape, jnp.bfloat16)
    last_shape = jax.ShapeDtypeStruct((2, *frames.shape[1:]), jnp.bfloat16)
    head_shape = jax.ShapeDtypeStruct((depth - 2, *frames.shape[1:]), jnp.bfloat16)

    active_shape = jax.ShapeDtypeStruct((depth + 2, height, columns, channels), jnp.bfloat16)
    inner_shape = jax.ShapeDtypeStruct((depth, height - 2, columns, channels), jnp.bfloat16)
    totals_shape = jax.ShapeDtypeStruct((2, 8, channels), jnp.float32)

    def halo(count):
        return pltpu.VMEM((count + 2, 2, columns, channels), jnp.bfloat16)

    def call(kernel, outs, inputs, count, scratch=(), hbm=(), out_specs=None):
        flops = 27 * count * height * columns * channels * channels
        return pl.pallas_call(
            kernel, out_shape=outs, in_specs=[HBM if i in hbm else VMEM for i in range(len(inputs))],
            out_specs=out_specs or (VMEM,) * len(outs), scratch_shapes=list(scratch),
            compiler_params=params(24),
            cost_estimate=pl.CostEstimate(flops=flops, bytes_accessed=8 << 20, transcendentals=0),
        )(*inputs)

    row_shape = jax.ShapeDtypeStruct((depth, columns, channels), jnp.bfloat16)

    def padded(count):
        return pltpu.VMEM((count + 2, height + 2, columns, channels), jnp.bfloat16)

    stats, head, last, near, far = call(
        stats_kernel, (stats_shape, head_shape, last_shape, row_shape, row_shape),
        (frames,), 2,
    )
    past = sent_ahead(last)
    near, far = sent_sideways(near, far)
    stats = exchange(stats)
    corner = sent_sideways(*pick((past,), stats))
    around = (past, *corner)
    own = (head, last, near, far, stats, first_gain[None], first_bias[None], first_weight)
    alone = depth >= 4
    ahead = (() if alone else around) + own
    last, totals = call(
        functools.partial(first_kernel, members, depth - 2, 2, not alone),
        (last_shape, totals_shape), ahead, 2, (padded(2),),
    )
    head, stats = call(
        functools.partial(first_kernel, members, 0, depth - 2, True),
        (head_shape, stats_shape), (*around, *own, totals), depth - 2, (padded(depth - 2),),
    )
    past = sent_ahead(last)
    stats = exchange(stats)
    near, far = sent_sideways(*pick((past, head, last), stats))
    norm = (stats, second_gain[None], second_bias[None], second_weight)
    active, inside = call(
        functools.partial(inner_second, members),
        (active_shape, inner_shape), (past, head, last, *norm, frames), depth,
    )
    features, patches = call(
        functools.partial(outer_second, members),
        (cells_shape, jax.ShapeDtypeStruct((parts, rows, LANES), jnp.bfloat16)),
        (near, far, active, *norm, inside, frames, latent_weight.T), depth,
        (halo(depth), pltpu.VMEM(frames.shape, jnp.bfloat16),
         pltpu.VMEM((depth, height * columns, LANES), jnp.float32),
         pltpu.VMEM((parts, rows, LANES), jnp.float32), pltpu.SemaphoreType.DMA((3,))),
        (), (HBM, VMEM),
    )
    received = lax.all_to_all(patches, "tile", split_axis=0, concat_axis=0, tiled=True)
    tokens = pl.pallas_call(
        functools.partial(unpack_kernel, blocks, pairs),
        out_shape=jax.ShapeDtypeStruct((depth, parts * pairs, blocks * LANES), jnp.bfloat16),
        in_specs=[VMEM], out_specs=VMEM,
        scratch_shapes=[pltpu.VMEM((parts * rows, LANES), jnp.float32),
                        pltpu.VMEM((depth * blocks, parts * pairs, LANES), jnp.float32)],
        compiler_params=params(16), name="unpack",
    )(received)
    return features, tokens


def solution(mesh):
    in_specs = (P("tm", "tile", None, None), P(), P(), P(), P(), P(), P(), P())
    out_specs = (P("tm", "tile", None, None), P("tm", None, "tile"))
    return jax.shard_map(body, mesh=mesh, in_specs=in_specs, out_specs=out_specs, check_vma=False)
```

```python
import functools

import jax
import jax.numpy as jnp
from jax import lax
from jax.experimental import pallas as pl
from jax.experimental.pallas import tpu as pltpu
from jax.sharding import PartitionSpec as P


GROUPS = 32
ALL = ("tm", "tile")
VMEM = pl.BlockSpec(memory_space=pltpu.VMEM)
HBM = pl.BlockSpec(memory_space=pltpu.HBM)
LANES = 128


def params(mib):
    return pltpu.CompilerParams(vmem_limit_bytes=mib << 20)


def row_totals(value):
    folded = value.reshape(-1, 8, value.shape[-1])
    return jnp.sum(folded, axis=0)


def put_stats(out_ref, sums, squares):
    pair = jnp.concatenate(
        [jnp.sum(sums, axis=0, keepdims=True), jnp.sum(squares, axis=0, keepdims=True)], axis=0
    )
    out_ref[...] = jnp.broadcast_to(pair[None], out_ref.shape)


def sides(height):
    even = lax.axis_index("tile") % 2 == 0
    return jnp.where(even, height - 1, 0), jnp.where(even, 0, height - 1)


def take_kernel(frames_hbm, last_ref, sem):
    depth = frames_hbm.shape[0]
    copy = pltpu.make_async_copy(frames_hbm.at[depth - 2 :], last_ref, sem)
    copy.start()
    copy.wait()


def stats_kernel(frames_hbm, last_ref, out_ref, head_ref, near_ref, far_ref, sem):
    before, height, _, channels = head_ref.shape
    near, far = sides(height)
    load = pltpu.make_async_copy(frames_hbm.at[:before], head_ref, sem)
    load.start()

    def totals(ref, shift, carry):
        def step(t, carry):
            sums, squares = carry
            for h in range(height):
                value = ref[t, h].astype(jnp.float32)
                sums = sums + row_totals(value)
                squares = squares + row_totals(value * value)
            near_ref[shift + t] = ref[t, near]
            far_ref[shift + t] = ref[t, far]
            return sums, squares

        return lax.fori_loop(0, ref.shape[0], step, carry)

    zero = jnp.zeros((8, channels), jnp.float32)
    carry = totals(last_ref, before, (zero, zero))
    load.wait()
    sums, squares = totals(head_ref, 0, carry)
    put_stats(out_ref, sums, squares)


def pick_kernel(count, *refs):
    cell_refs, (near_ref, far_ref) = refs[:count], refs[-2:]
    near, far = sides(cell_refs[0].shape[1])
    t = 0
    for ref in cell_refs:
        for frame in range(ref.shape[0]):
            near_ref[t] = ref[frame, near]
            far_ref[t] = ref[frame, far]
            t += 1


def group_sum(value, size):
    channels = value.shape[1]
    lane = lax.broadcasted_iota(jnp.int32, value.shape, 1)
    step = 1
    while step < size:
        ahead = pltpu.roll(value, channels - step, 1)
        behind = pltpu.roll(value, step, 1)
        value = value + jnp.where((lane // step) % 2 == 0, ahead, behind)
        step *= 2
    return value


def scale_of(stats_ref, gain_ref, bias_ref, members):
    channels = stats_ref.shape[2]
    totals = jnp.sum(stats_ref[...], axis=0)
    totals = jnp.concatenate([totals, jnp.zeros((6, channels), jnp.float32)], axis=0)
    totals = group_sum(totals, channels // GROUPS)
    average = totals[0:1] / members
    spread = totals[1:2] / members - average * average
    factor = lax.rsqrt(spread + 1e-06) * gain_ref[...]
    return factor, bias_ref[...] - average * factor


def silu(value):
    return value * (0.5 * jnp.tanh(0.5 * value) + 0.5)


def activate(value, scale, keep):
    factor, offset = scale
    active = silu(value.astype(jnp.float32) * factor + offset)
    if keep is not None:
        active = active * keep
    return active.astype(jnp.bfloat16)


def has_past():
    return (lax.axis_index("tm") > 0).astype(jnp.float32)


def convolve(piece, weight_ref, columns, taps=None):
    taps = taps or [(a, b) for a in range(3) for b in range(3)]
    totals = []
    for c in range(3):
        total = None
        for a, b in taps:
            part = jnp.dot(piece(a, b), weight_ref[a, b, c], preferred_element_type=jnp.float32)
            total = part if total is None else total + part
        totals.append(total)
    rows = totals[0].shape[0]
    column = lax.broadcasted_iota(jnp.int32, totals[0].shape, 0) % columns
    left = jnp.where(column == 0, 0.0, pltpu.roll(totals[0], 1, 0))
    right = jnp.where(column == columns - 1, 0.0, pltpu.roll(totals[2], rows - 1, 0))
    return totals[1] + left + right


def steps(count):
    return [(t, min(2, count - t)) for t in range(0, count, 2)]


def edges(active_ref, scale):
    index, count = lax.axis_index("tile"), lax.axis_size("tile")
    height = active_ref.shape[1] - 2
    even = index % 2 == 0
    first = (lax.axis_index("tm") > 0).astype(jnp.float32)
    above = (index > 0).astype(jnp.float32)
    below = (index < count - 1).astype(jnp.float32)
    factor, offset = scale

    def put(t, h, value, keep):
        active = silu(value.astype(jnp.float32) * factor + offset)
        if keep is not None:
            active = active * keep
        active_ref[t, h] = active.astype(jnp.bfloat16)

    def fill(t, source):
        cells, near, far, is_past = source
        near, far = near[...], far[...]
        put(t, 0, jnp.where(even, far, near), above * first if is_past else above)
        for h in range(height):
            put(t, h + 1, cells[h], first if is_past else None)
        put(t, height + 1, jnp.where(even, near, far), below * first if is_past else below)

    return fill


def sources(pieces):
    found = []
    for cells, near, far, is_past in pieces:
        row = 0
        for ref in cells:
            for t in range(ref.shape[0]):
                found.append((ref.at[t], near.at[row], far.at[row], is_past))
                row += 1
    return found


def split(refs, with_past):
    refs = list(refs)
    pieces = [((refs.pop(0),), refs.pop(0), refs.pop(0), True)] if with_past else []
    head, last, near, far = refs[:4]
    pieces.append(((head, last), near, far, False))
    return sources(pieces), refs[4:]


def first_kernel(members, begin, count, with_past, *refs):
    found, refs = split(refs, with_past)
    found = found if with_past else [None, None, *found]
    stats, gain, bias, weight = refs[:4]
    active_ref = refs[-1]
    height, columns, channels = active_ref.shape[1] - 2, *active_ref.shape[2:]
    fill = edges(active_ref, scale_of(stats, gain, bias, members))
    if begin == 0:
        totals, hidden_ref, totals_ref = refs[4:-1]
        sums, squares = totals[0], totals[1]
    else:
        hidden_ref, totals_ref = refs[4:-1]
        sums = squares = jnp.zeros((8, channels), jnp.float32)
    for t in range(2):
        fill(t, found[begin + t])
    for t in range(count):
        fill(t + 2, found[begin + t + 2])

        def piece(a, b, t=t):
            return active_ref[t + a, b : b + height].reshape(height * columns, channels)

        hidden = convolve(piece, weight, columns).astype(jnp.bfloat16)
        wide = hidden.astype(jnp.float32)
        sums = sums + row_totals(wide)
        squares = squares + row_totals(wide * wide)
        hidden_ref[t] = hidden.reshape(height, columns, channels)
    if begin == 0:
        put_stats(totals_ref, sums, squares)
    else:
        totals_ref[0] = sums
        totals_ref[1] = squares


def inner(members, past, head, last, stats, gain, bias, weight, active_ref, partial_ref, finish):
    height, columns, channels = active_ref.shape[1:]
    scale = scale_of(stats, gain, bias, members)
    first = has_past()
    found = [(ref.at[t], ref is past) for ref in (past, head, last) for t in range(ref.shape[0])]
    done = 0
    for t, count in steps(len(found) - 2):
        while done < t + count + 2:
            cells, is_past = found[done]
            for h in range(height):
                active_ref[done, h] = activate(cells[h], scale, first if is_past else None)
            done += 1

        def piece(a, b, t=t, count=count):
            cells = active_ref[t + a : t + a + count, b : b + height - 2]
            return cells.reshape(count * (height - 2) * columns, channels)

        finish(t, count, convolve(piece, weight, columns))

    depth = len(found) - 2
    for edge, shift in enumerate((-1, height - 2)):

        def own(a, b, shift=shift):
            return active_ref[a : a + depth, shift + b].reshape(depth * columns, channels)

        taps = [(a, b) for a in range(3) for b in range(3) if 0 <= shift + b < height]
        partial_ref[edge] = convolve(own, weight, columns, taps)


def inner_second(members, past, head, last, stats, gain, bias, weight, frames,
                 inner_ref, partial_ref, active_ref):
    height = frames.shape[1]

    def finish(t, count, total):
        cells = frames[t : t + count, 1 : height - 1].astype(jnp.float32).reshape(total.shape)
        inner_ref[t : t + count] = (cells + total).astype(jnp.bfloat16).reshape(
            count, *inner_ref.shape[1:]
        )

    inner(members, past, head, last, stats, gain, bias, weight, active_ref, partial_ref, finish)


def outer(members, near, far, stats, gain, bias, weight, partial, halo_ref):
    columns, channels = halo_ref.shape[2:]
    depth = halo_ref.shape[0] - 2
    scale = scale_of(stats, gain, bias, members)
    index, count = lax.axis_index("tile"), lax.axis_size("tile")
    even = index % 2 == 0
    first = has_past()
    above = (index > 0).astype(jnp.float32)
    below = (index < count - 1).astype(jnp.float32)
    for t in range(depth + 2):
        rows = near[t], far[t]
        top, bottom = (above * first, below * first) if t < 2 else (above, below)
        halo_ref[t, 0] = activate(jnp.where(even, rows[1], rows[0]), scale, top)
        halo_ref[t, 1] = activate(jnp.where(even, rows[0], rows[1]), scale, bottom)
    totals = []
    for edge in range(2):

        def piece(a, b, edge=edge):
            return halo_ref[a : a + depth, edge].reshape(depth * columns, channels)

        taps = [(a, 2 * edge) for a in range(3)]
        totals.append(partial[edge] + convolve(piece, weight, columns, taps))
    return totals


def outer_second(members, near, far, stats, gain, bias, weight, inside, partial, frames, latent,
                 features_hbm, patches_ref, halo_ref, cells_ref, latents_ref, packed_ref, sem):
    depth, height, columns, channels = cells_ref.shape
    stores = [pltpu.make_async_copy(inside, features_hbm.at[:, 1 : height - 1], sem.at[2])]
    stores[0].start()
    width = LANES // 8
    parts, rows = packed_ref.shape[:2]
    pairs = height // 2
    blocks = rows // (depth * pairs)
    lane = lax.broadcasted_iota(jnp.int32, (columns // 4, LANES), 1) // width
    spread = lax.broadcasted_iota(jnp.int32, (width, LANES), 0) == (
        lax.broadcasted_iota(jnp.int32, (width, LANES), 1) % width
    )
    wide_latent = lax.dot_general(
        latent[...], spread.astype(jnp.bfloat16), (((0,), (0,)), ((), ())),
        preferred_element_type=jnp.float32,
    ).astype(jnp.bfloat16)
    cells_ref[:, 1 : height - 1] = inside[...]

    totals = outer(members, near, far, stats, gain, bias, weight, partial, halo_ref)
    for total, h in zip(totals, (0, height - 1)):
        branch = total.reshape(depth, columns, channels)
        for t in range(depth):
            cells_ref[t, h] = (frames[t, h].astype(jnp.float32) + branch[t]).astype(jnp.bfloat16)
    for n, h in enumerate((0, height - 1)):
        stores.append(
            pltpu.make_async_copy(
                cells_ref.at[:, h : h + 1], features_hbm.at[:, h : h + 1], sem.at[n]
            )
        )
        stores[-1].start()
    for t in range(depth):
        latents_ref[t] = (
            jnp.dot(
                cells_ref[t].reshape(height * columns, channels), wide_latent,
                preferred_element_type=jnp.float32,
            )
            .astype(jnp.bfloat16)
            .astype(jnp.float32)
        )
    for t in range(depth):
        for i in range(pairs):
            mixed = None
            for cell in range(8):
                j, p, q = cell // 4, cell // 2 % 2, cell % 2
                start = (2 * i + p) * columns + 2 * j + q
                value = latents_ref[t, pl.ds(start, columns // 4, stride=4), :]
                mixed = value if mixed is None else jnp.where(lane == cell, value, mixed)
            for d in range(parts):
                packed_ref[d, pl.ds(t * blocks * pairs + i, blocks, stride=pairs), :] = mixed[
                    d * blocks : (d + 1) * blocks
                ]
    patches_ref[...] = packed_ref[...].astype(jnp.bfloat16)
    for store in stores:
        store.wait()


def unpack_kernel(blocks, pairs, received, tokens_ref, flat_ref, mixed_ref):
    parts, rows, lanes = received.shape
    flat_ref[...] = received[...].astype(jnp.float32).reshape(parts * rows, lanes)
    depth = rows // (blocks * pairs)
    for t in range(depth):
        for block in range(blocks):
            for i in range(pairs):
                start = (t * blocks + block) * pairs + i
                mixed_ref[t * blocks + block, pl.ds(i, parts, stride=pairs), :] = flat_ref[
                    pl.ds(start, parts, stride=rows), :
                ]
            tokens_ref[t, :, block * lanes : (block + 1) * lanes] = mixed_ref[
                t * blocks + block
            ].astype(jnp.bfloat16)


def sent_ahead(last):
    pairs = [(i, i + 1) for i in range(lax.axis_size("tm") - 1)]
    return lax.ppermute(last, "tm", pairs)


def sent_sideways(near, far):
    count = lax.axis_size("tile")
    near_pairs = [(i, i ^ 1) for i in range(count) if i ^ 1 < count]
    far_pairs = [pair for i in range(1, count - 1, 2) for pair in ((i, i + 1), (i + 1, i))]
    near = lax.ppermute(near, "tile", near_pairs)
    far = lax.ppermute(far, "tile", far_pairs)
    return near, far


def pick(cells, *after):
    rows = sum(piece.shape[0] for piece in cells)
    rows = jax.ShapeDtypeStruct((rows, *cells[0].shape[2:]), jnp.bfloat16)
    return pl.pallas_call(
        functools.partial(pick_kernel, len(cells)), out_shape=(rows, rows),
        in_specs=[VMEM] * len(cells) + [pl.BlockSpec(memory_space=pl.ANY)] * len(after),
        out_specs=(VMEM, VMEM), compiler_params=params(8), name="pick",
    )(*cells, *after)


def exchange(stats):
    return lax.all_to_all(stats, ALL, split_axis=0, concat_axis=0, tiled=True)


def body(frames, first_gain, first_bias, first_weight, second_gain, second_bias, second_weight,
         latent_weight):
    depth, height, columns, channels = frames.shape
    parts = lax.axis_size("tile")
    devices = lax.axis_size("tm") * parts
    members = float(devices * depth * height * columns * (channels // GROUPS))
    latent_width = latent_weight.shape[1]
    pairs = height // 2
    blocks = columns // 2 * 4 * latent_width // parts // LANES
    rows = depth * blocks * pairs
    stats_shape = jax.ShapeDtypeStruct((devices, 2, channels), jnp.float32)
    cells_shape = jax.ShapeDtypeStruct(frames.shape, jnp.bfloat16)
    last_shape = jax.ShapeDtypeStruct((2, *frames.shape[1:]), jnp.bfloat16)
    head_shape = jax.ShapeDtypeStruct((depth - 2, *frames.shape[1:]), jnp.bfloat16)

    active_shape = jax.ShapeDtypeStruct((depth + 2, height, columns, channels), jnp.bfloat16)
    inner_shape = jax.ShapeDtypeStruct((depth, height - 2, columns, channels), jnp.bfloat16)
    partial_shape = jax.ShapeDtypeStruct((2, depth * columns, channels), jnp.float32)
    totals_shape = jax.ShapeDtypeStruct((2, 8, channels), jnp.float32)

    def halo(count):
        return pltpu.VMEM((count + 2, 2, columns, channels), jnp.bfloat16)

    def call(kernel, outs, inputs, count, scratch=(), hbm=(), out_specs=None):
        flops = 27 * count * height * columns * channels * channels
        return pl.pallas_call(
            kernel, out_shape=outs, in_specs=[HBM if i in hbm else VMEM for i in range(len(inputs))],
            out_specs=out_specs or (VMEM,) * len(outs), scratch_shapes=list(scratch),
            compiler_params=params(24),
            cost_estimate=pl.CostEstimate(flops=flops, bytes_accessed=8 << 20, transcendentals=0),
        )(*inputs)

    row_shape = jax.ShapeDtypeStruct((depth, columns, channels), jnp.bfloat16)

    def padded(count):
        return pltpu.VMEM((count + 2, height + 2, columns, channels), jnp.bfloat16)

    cells = pltpu.with_memory_space_constraint(frames, pltpu.HBM)
    (last,) = call(take_kernel, (last_shape,), (cells,), 1, (pltpu.SemaphoreType.DMA(()),), (0,))
    past = sent_ahead(last)
    stats, head, near, far = call(
        stats_kernel, (stats_shape, head_shape, row_shape, row_shape),
        (cells, last), 2, (pltpu.SemaphoreType.DMA(()),), (0,),
    )
    near, far = sent_sideways(near, far)
    stats = exchange(stats)
    corner = sent_sideways(*pick((past,), stats))
    around = (past, *corner)
    own = (head, last, near, far, stats, first_gain[None], first_bias[None], first_weight)
    alone = depth >= 4
    ahead = (() if alone else around) + own
    last, totals = call(
        functools.partial(first_kernel, members, depth - 2, 2, not alone),
        (last_shape, totals_shape), ahead, 2, (padded(2),),
    )
    head, stats = call(
        functools.partial(first_kernel, members, 0, depth - 2, True),
        (head_shape, stats_shape), (*around, *own, totals), depth - 2, (padded(depth - 2),),
    )
    past = sent_ahead(last)
    stats = exchange(stats)
    near, far = sent_sideways(*pick((past, head, last), stats))
    norm = (stats, second_gain[None], second_bias[None], second_weight)
    inside, partial = call(
        functools.partial(inner_second, members),
        (inner_shape, partial_shape), (past, head, last, *norm, frames), depth,
        (pltpu.VMEM(active_shape.shape, jnp.bfloat16),),
    )
    features, patches = call(
        functools.partial(outer_second, members),
        (cells_shape, jax.ShapeDtypeStruct((parts, rows, LANES), jnp.bfloat16)),
        (near, far, *norm, inside, partial, frames, latent_weight.T), depth,
        (halo(depth), pltpu.VMEM(frames.shape, jnp.bfloat16),
         pltpu.VMEM((depth, height * columns, LANES), jnp.float32),
         pltpu.VMEM((parts, rows, LANES), jnp.float32), pltpu.SemaphoreType.DMA((3,))),
        (), (HBM, VMEM),
    )
    received = lax.all_to_all(patches, "tile", split_axis=0, concat_axis=0, tiled=True)
    tokens = pl.pallas_call(
        functools.partial(unpack_kernel, blocks, pairs),
        out_shape=jax.ShapeDtypeStruct((depth, parts * pairs, blocks * LANES), jnp.bfloat16),
        in_specs=[VMEM], out_specs=VMEM,
        scratch_shapes=[pltpu.VMEM((parts * rows, LANES), jnp.float32),
                        pltpu.VMEM((depth * blocks, parts * pairs, LANES), jnp.float32)],
        compiler_params=params(16), name="unpack",
    )(received)
    return features, tokens


def solution(mesh):
    in_specs = (P("tm", "tile", None, None), P(), P(), P(), P(), P(), P(), P())
    out_specs = (P("tm", "tile", None, None), P("tm", None, "tile"))
    return jax.shard_map(body, mesh=mesh, in_specs=in_specs, out_specs=out_specs, check_vma=False)
```

```python
import functools

import jax
import jax.numpy as jnp
from jax import lax
from jax.experimental import pallas as pl
from jax.experimental.pallas import tpu as pltpu
from jax.sharding import PartitionSpec as P


GROUPS = 32
ALL = ("tm", "tile")
VMEM = pl.BlockSpec(memory_space=pltpu.VMEM)
HBM = pl.BlockSpec(memory_space=pltpu.HBM)
LANES = 128


def params(mib):
    return pltpu.CompilerParams(vmem_limit_bytes=mib << 20)


def row_totals(value):
    folded = value.reshape(-1, 8, value.shape[-1])
    return jnp.sum(folded, axis=0)


def put_stats(out_ref, sums, squares):
    pair = jnp.concatenate(
        [jnp.sum(sums, axis=0, keepdims=True), jnp.sum(squares, axis=0, keepdims=True)], axis=0
    )
    out_ref[...] = jnp.broadcast_to(pair[None], out_ref.shape)


def sides(height):
    even = lax.axis_index("tile") % 2 == 0
    return jnp.where(even, height - 1, 0), jnp.where(even, 0, height - 1)


def stats_kernel(frames_hbm, out_ref, head_ref, last_ref, near_ref, far_ref, sem):
    before, height, _, channels = head_ref.shape
    near, far = sides(height)
    loads = [
        pltpu.make_async_copy(frames_hbm.at[before + t], last_ref.at[t], sem.at[before + t])
        for t in range(last_ref.shape[0])
    ]
    loads += [
        pltpu.make_async_copy(frames_hbm.at[t], head_ref.at[t], sem.at[t]) for t in range(before)
    ]
    for load in loads:
        load.start()

    def totals(ref, shift, carry):
        def step(t, carry):
            sums, squares = carry
            for h in range(height):
                value = ref[t, h].astype(jnp.float32)
                sums = sums + row_totals(value)
                squares = squares + row_totals(value * value)
            near_ref[shift + t] = ref[t, near]
            far_ref[shift + t] = ref[t, far]
            return sums, squares

        for t in range(ref.shape[0]):
            loads[order.pop(0)].wait()
            carry = step(t, carry)
        return carry

    order = list(range(len(loads)))
    zero = jnp.zeros((8, channels), jnp.float32)
    carry = totals(last_ref, before, (zero, zero))
    sums, squares = totals(head_ref, 0, carry)
    put_stats(out_ref, sums, squares)


def pick_kernel(count, *refs):
    cell_refs, (near_ref, far_ref) = refs[:count], refs[-2:]
    near, far = sides(cell_refs[0].shape[1])
    t = 0
    for ref in cell_refs:
        for frame in range(ref.shape[0]):
            near_ref[t] = ref[frame, near]
            far_ref[t] = ref[frame, far]
            t += 1


def group_sum(value, size):
    channels = value.shape[1]
    lane = lax.broadcasted_iota(jnp.int32, value.shape, 1)
    step = 1
    while step < size:
        ahead = pltpu.roll(value, channels - step, 1)
        behind = pltpu.roll(value, step, 1)
        value = value + jnp.where((lane // step) % 2 == 0, ahead, behind)
        step *= 2
    return value


def scale_of(stats_ref, gain_ref, bias_ref, members):
    channels = stats_ref.shape[2]
    totals = jnp.sum(stats_ref[...], axis=0)
    totals = jnp.concatenate([totals, jnp.zeros((6, channels), jnp.float32)], axis=0)
    totals = group_sum(totals, channels // GROUPS)
    average = totals[0:1] / members
    spread = totals[1:2] / members - average * average
    factor = lax.rsqrt(spread + 1e-06) * gain_ref[...]
    return factor, bias_ref[...] - average * factor


def silu(value):
    return value * (0.5 * jnp.tanh(0.5 * value) + 0.5)


def activate(value, scale, keep):
    factor, offset = scale
    active = silu(value.astype(jnp.float32) * factor + offset)
    if keep is not None:
        active = active * keep
    return active.astype(jnp.bfloat16)


def has_past():
    return (lax.axis_index("tm") > 0).astype(jnp.float32)


def convolve(piece, weight_ref, columns, taps=None):
    taps = taps or [(a, b) for a in range(3) for b in range(3)]
    totals = []
    for c in range(3):
        total = None
        for a, b in taps:
            part = jnp.dot(piece(a, b), weight_ref[a, b, c], preferred_element_type=jnp.float32)
            total = part if total is None else total + part
        totals.append(total)
    rows = totals[0].shape[0]
    column = lax.broadcasted_iota(jnp.int32, totals[0].shape, 0) % columns
    left = jnp.where(column == 0, 0.0, pltpu.roll(totals[0], 1, 0))
    right = jnp.where(column == columns - 1, 0.0, pltpu.roll(totals[2], rows - 1, 0))
    return totals[1] + left + right


def steps(count):
    return [(t, min(2, count - t)) for t in range(0, count, 2)]


def edges(active_ref, scale):
    index, count = lax.axis_index("tile"), lax.axis_size("tile")
    height = active_ref.shape[1] - 2
    even = index % 2 == 0
    first = (lax.axis_index("tm") > 0).astype(jnp.float32)
    above = (index > 0).astype(jnp.float32)
    below = (index < count - 1).astype(jnp.float32)
    factor, offset = scale

    def put(t, h, value, keep):
        active = silu(value.astype(jnp.float32) * factor + offset)
        if keep is not None:
            active = active * keep
        active_ref[t, h] = active.astype(jnp.bfloat16)

    def fill(t, source):
        cells, near, far, is_past = source
        near, far = near[...], far[...]
        put(t, 0, jnp.where(even, far, near), above * first if is_past else above)
        for h in range(height):
            put(t, h + 1, cells[h], first if is_past else None)
        put(t, height + 1, jnp.where(even, near, far), below * first if is_past else below)

    return fill


def sources(pieces):
    found = []
    for cells, near, far, is_past in pieces:
        row = 0
        for ref in cells:
            for t in range(ref.shape[0]):
                found.append((ref.at[t], near.at[row], far.at[row], is_past))
                row += 1
    return found


def split(refs, with_past):
    refs = list(refs)
    pieces = [((refs.pop(0),), refs.pop(0), refs.pop(0), True)] if with_past else []
    head, last, near, far = refs[:4]
    pieces.append(((head, last), near, far, False))
    return sources(pieces), refs[4:]


def first_kernel(members, begin, count, with_past, *refs):
    found, refs = split(refs, with_past)
    found = found if with_past else [None, None, *found]
    stats, gain, bias, weight = refs[:4]
    active_ref = refs[-1]
    height, columns, channels = active_ref.shape[1] - 2, *active_ref.shape[2:]
    fill = edges(active_ref, scale_of(stats, gain, bias, members))
    if begin == 0:
        totals, hidden_ref, totals_ref = refs[4:-1]
        sums, squares = totals[0], totals[1]
    else:
        hidden_ref, totals_ref = refs[4:-1]
        sums = squares = jnp.zeros((8, channels), jnp.float32)
    for t in range(2):
        fill(t, found[begin + t])
    for t in range(count):
        fill(t + 2, found[begin + t + 2])

        def piece(a, b, t=t):
            return active_ref[t + a, b : b + height].reshape(height * columns, channels)

        hidden = convolve(piece, weight, columns).astype(jnp.bfloat16)
        wide = hidden.astype(jnp.float32)
        sums = sums + row_totals(wide)
        squares = squares + row_totals(wide * wide)
        hidden_ref[t] = hidden.reshape(height, columns, channels)
    if begin == 0:
        put_stats(totals_ref, sums, squares)
    else:
        totals_ref[0] = sums
        totals_ref[1] = squares


def inner(members, past, head, last, stats, gain, bias, weight, active_ref, partial_ref, finish):
    height, columns, channels = active_ref.shape[1:]
    scale = scale_of(stats, gain, bias, members)
    first = has_past()
    found = [(ref.at[t], ref is past) for ref in (past, head, last) for t in range(ref.shape[0])]
    done = 0
    for t, count in steps(len(found) - 2):
        while done < t + count + 2:
            cells, is_past = found[done]
            for h in range(height):
                active_ref[done, h] = activate(cells[h], scale, first if is_past else None)
            done += 1

        def piece(a, b, t=t, count=count):
            cells = active_ref[t + a : t + a + count, b : b + height - 2]
            return cells.reshape(count * (height - 2) * columns, channels)

        finish(t, count, convolve(piece, weight, columns))

    depth = len(found) - 2
    for edge, shift in enumerate((-1, height - 2)):

        def own(a, b, shift=shift):
            return active_ref[a : a + depth, shift + b].reshape(depth * columns, channels)

        taps = [(a, b) for a in range(3) for b in range(3) if 0 <= shift + b < height]
        partial_ref[edge] = convolve(own, weight, columns, taps)


def inner_second(members, past, head, last, stats, gain, bias, weight, frames,
                 inner_ref, partial_ref, active_ref):
    height = frames.shape[1]

    def finish(t, count, total):
        cells = frames[t : t + count, 1 : height - 1].astype(jnp.float32).reshape(total.shape)
        inner_ref[t : t + count] = (cells + total).astype(jnp.bfloat16).reshape(
            count, *inner_ref.shape[1:]
        )

    inner(members, past, head, last, stats, gain, bias, weight, active_ref, partial_ref, finish)


def outer(members, near, far, stats, gain, bias, weight, partial, halo_ref):
    columns, channels = halo_ref.shape[2:]
    depth = halo_ref.shape[0] - 2
    scale = scale_of(stats, gain, bias, members)
    index, count = lax.axis_index("tile"), lax.axis_size("tile")
    even = index % 2 == 0
    first = has_past()
    above = (index > 0).astype(jnp.float32)
    below = (index < count - 1).astype(jnp.float32)
    for t in range(depth + 2):
        rows = near[t], far[t]
        top, bottom = (above * first, below * first) if t < 2 else (above, below)
        halo_ref[t, 0] = activate(jnp.where(even, rows[1], rows[0]), scale, top)
        halo_ref[t, 1] = activate(jnp.where(even, rows[0], rows[1]), scale, bottom)
    totals = []
    for edge in range(2):

        def piece(a, b, edge=edge):
            return halo_ref[a : a + depth, edge].reshape(depth * columns, channels)

        taps = [(a, 2 * edge) for a in range(3)]
        totals.append(partial[edge] + convolve(piece, weight, columns, taps))
    return totals


def outer_second(members, near, far, stats, gain, bias, weight, inside, partial, frames, latent,
                 features_hbm, patches_ref, halo_ref, cells_ref, latents_ref, packed_ref, sem):
    depth, height, columns, channels = cells_ref.shape
    stores = [pltpu.make_async_copy(inside, features_hbm.at[:, 1 : height - 1], sem.at[2])]
    stores[0].start()
    width = LANES // 8
    parts, rows = packed_ref.shape[:2]
    pairs = height // 2
    blocks = rows // (depth * pairs)
    lane = lax.broadcasted_iota(jnp.int32, (columns // 4, LANES), 1) // width
    spread = lax.broadcasted_iota(jnp.int32, (width, LANES), 0) == (
        lax.broadcasted_iota(jnp.int32, (width, LANES), 1) % width
    )
    wide_latent = lax.dot_general(
        latent[...], spread.astype(jnp.bfloat16), (((0,), (0,)), ((), ())),
        preferred_element_type=jnp.float32,
    ).astype(jnp.bfloat16)
    cells_ref[:, 1 : height - 1] = inside[...]

    totals = outer(members, near, far, stats, gain, bias, weight, partial, halo_ref)
    for total, h in zip(totals, (0, height - 1)):
        branch = total.reshape(depth, columns, channels)
        for t in range(depth):
            cells_ref[t, h] = (frames[t, h].astype(jnp.float32) + branch[t]).astype(jnp.bfloat16)
    for n, h in enumerate((0, height - 1)):
        stores.append(
            pltpu.make_async_copy(
                cells_ref.at[:, h : h + 1], features_hbm.at[:, h : h + 1], sem.at[n]
            )
        )
        stores[-1].start()
    for t in range(depth):
        latents_ref[t] = (
            jnp.dot(
                cells_ref[t].reshape(height * columns, channels), wide_latent,
                preferred_element_type=jnp.float32,
            )
            .astype(jnp.bfloat16)
            .astype(jnp.float32)
        )
    for t in range(depth):
        for i in range(pairs):
            mixed = None
            for cell in range(8):
                j, p, q = cell // 4, cell // 2 % 2, cell % 2
                start = (2 * i + p) * columns + 2 * j + q
                value = latents_ref[t, pl.ds(start, columns // 4, stride=4), :]
                mixed = value if mixed is None else jnp.where(lane == cell, value, mixed)
            for d in range(parts):
                packed_ref[d, pl.ds(t * blocks * pairs + i, blocks, stride=pairs), :] = mixed[
                    d * blocks : (d + 1) * blocks
                ]
    patches_ref[...] = packed_ref[...].astype(jnp.bfloat16)
    for store in stores:
        store.wait()


def unpack_kernel(blocks, pairs, received, tokens_ref, flat_ref, mixed_ref):
    parts, rows, lanes = received.shape
    flat_ref[...] = received[...].astype(jnp.float32).reshape(parts * rows, lanes)
    depth = rows // (blocks * pairs)
    for t in range(depth):
        for block in range(blocks):
            for i in range(pairs):
                start = (t * blocks + block) * pairs + i
                mixed_ref[t * blocks + block, pl.ds(i, parts, stride=pairs), :] = flat_ref[
                    pl.ds(start, parts, stride=rows), :
                ]
            tokens_ref[t, :, block * lanes : (block + 1) * lanes] = mixed_ref[
                t * blocks + block
            ].astype(jnp.bfloat16)


def sent_ahead(last):
    pairs = [(i, i + 1) for i in range(lax.axis_size("tm") - 1)]
    return lax.ppermute(last, "tm", pairs)


def sent_sideways(near, far):
    count = lax.axis_size("tile")
    near_pairs = [(i, i ^ 1) for i in range(count) if i ^ 1 < count]
    far_pairs = [pair for i in range(1, count - 1, 2) for pair in ((i, i + 1), (i + 1, i))]
    near = lax.ppermute(near, "tile", near_pairs)
    far = lax.ppermute(far, "tile", far_pairs)
    return near, far


def pick(cells, *after):
    rows = sum(piece.shape[0] for piece in cells)
    rows = jax.ShapeDtypeStruct((rows, *cells[0].shape[2:]), jnp.bfloat16)
    return pl.pallas_call(
        functools.partial(pick_kernel, len(cells)), out_shape=(rows, rows),
        in_specs=[VMEM] * len(cells) + [pl.BlockSpec(memory_space=pl.ANY)] * len(after),
        out_specs=(VMEM, VMEM), compiler_params=params(8), name="pick",
    )(*cells, *after)


def exchange(stats):
    return lax.all_to_all(stats, ALL, split_axis=0, concat_axis=0, tiled=True)


def body(frames, first_gain, first_bias, first_weight, second_gain, second_bias, second_weight,
         latent_weight):
    depth, height, columns, channels = frames.shape
    parts = lax.axis_size("tile")
    devices = lax.axis_size("tm") * parts
    members = float(devices * depth * height * columns * (channels // GROUPS))
    latent_width = latent_weight.shape[1]
    pairs = height // 2
    blocks = columns // 2 * 4 * latent_width // parts // LANES
    rows = depth * blocks * pairs
    stats_shape = jax.ShapeDtypeStruct((devices, 2, channels), jnp.float32)
    cells_shape = jax.ShapeDtypeStruct(frames.shape, jnp.bfloat16)
    last_shape = jax.ShapeDtypeStruct((2, *frames.shape[1:]), jnp.bfloat16)
    head_shape = jax.ShapeDtypeStruct((depth - 2, *frames.shape[1:]), jnp.bfloat16)

    active_shape = jax.ShapeDtypeStruct((depth + 2, height, columns, channels), jnp.bfloat16)
    inner_shape = jax.ShapeDtypeStruct((depth, height - 2, columns, channels), jnp.bfloat16)
    partial_shape = jax.ShapeDtypeStruct((2, depth * columns, channels), jnp.float32)
    totals_shape = jax.ShapeDtypeStruct((2, 8, channels), jnp.float32)

    def halo(count):
        return pltpu.VMEM((count + 2, 2, columns, channels), jnp.bfloat16)

    def call(kernel, outs, inputs, count, scratch=(), hbm=(), out_specs=None):
        flops = 27 * count * height * columns * channels * channels
        return pl.pallas_call(
            kernel, out_shape=outs, in_specs=[HBM if i in hbm else VMEM for i in range(len(inputs))],
            out_specs=out_specs or (VMEM,) * len(outs), scratch_shapes=list(scratch),
            compiler_params=params(24),
            cost_estimate=pl.CostEstimate(flops=flops, bytes_accessed=8 << 20, transcendentals=0),
        )(*inputs)

    row_shape = jax.ShapeDtypeStruct((depth, columns, channels), jnp.bfloat16)

    def padded(count):
        return pltpu.VMEM((count + 2, height + 2, columns, channels), jnp.bfloat16)

    cells = pltpu.with_memory_space_constraint(frames, pltpu.HBM)
    stats, head, last, near, far = call(
        stats_kernel, (stats_shape, head_shape, last_shape, row_shape, row_shape),
        (cells,), 2, (pltpu.SemaphoreType.DMA((depth,)),), (0,),
    )
    past = sent_ahead(last)
    near, far = sent_sideways(near, far)
    stats = exchange(stats)
    corner = sent_sideways(*pick((past,), stats))
    around = (past, *corner)
    own = (head, last, near, far, stats, first_gain[None], first_bias[None], first_weight)
    alone = depth >= 4
    ahead = (() if alone else around) + own
    last, totals = call(
        functools.partial(first_kernel, members, depth - 2, 2, not alone),
        (last_shape, totals_shape), ahead, 2, (padded(2),),
    )
    head, stats = call(
        functools.partial(first_kernel, members, 0, depth - 2, True),
        (head_shape, stats_shape), (*around, *own, totals), depth - 2, (padded(depth - 2),),
    )
    past = sent_ahead(last)
    stats = exchange(stats)
    near, far = sent_sideways(*pick((past, head, last), stats))
    norm = (stats, second_gain[None], second_bias[None], second_weight)
    inside, partial = call(
        functools.partial(inner_second, members),
        (inner_shape, partial_shape), (past, head, last, *norm, frames), depth,
        (pltpu.VMEM(active_shape.shape, jnp.bfloat16),),
    )
    features, patches = call(
        functools.partial(outer_second, members),
        (cells_shape, jax.ShapeDtypeStruct((parts, rows, LANES), jnp.bfloat16)),
        (near, far, *norm, inside, partial, frames, latent_weight.T), depth,
        (halo(depth), pltpu.VMEM(frames.shape, jnp.bfloat16),
         pltpu.VMEM((depth, height * columns, LANES), jnp.float32),
         pltpu.VMEM((parts, rows, LANES), jnp.float32), pltpu.SemaphoreType.DMA((3,))),
        (), (HBM, VMEM),
    )
    received = lax.all_to_all(patches, "tile", split_axis=0, concat_axis=0, tiled=True)
    tokens = pl.pallas_call(
        functools.partial(unpack_kernel, blocks, pairs),
        out_shape=jax.ShapeDtypeStruct((depth, parts * pairs, blocks * LANES), jnp.bfloat16),
        in_specs=[VMEM], out_specs=VMEM,
        scratch_shapes=[pltpu.VMEM((parts * rows, LANES), jnp.float32),
                        pltpu.VMEM((depth * blocks, parts * pairs, LANES), jnp.float32)],
        compiler_params=params(16), name="unpack",
    )(received)
    return features, tokens


def solution(mesh):
    in_specs = (P("tm", "tile", None, None), P(), P(), P(), P(), P(), P(), P())
    out_specs = (P("tm", "tile", None, None), P("tm", None, "tile"))
    return jax.shard_map(body, mesh=mesh, in_specs=in_specs, out_specs=out_specs, check_vma=False)
```
